512 devices in a mesh: lat: 64 (over z, x), tm: 8 (over y, core).
Axes of the slice: x: 4, y: 4, z: 16, core: 2. Of those that a mesh axis runs over, the one named last changes fastest.
Arguments:
- fields: bfloat16 [512, 256, 1024], P('lat', 'tm'), may hold values from -16 to 16
Outputs:
- covariance: float32 [256, 256], P('tm')
The draws below stay inside these ranges and needn't reach their ends.
All inputs are finite; a program needn't handle non-finite values.
Results may differ from the reference program's by a relative error of at most 0.0003.
Values may be sent and summed in bfloat16 or wider, within the bound.
A program may use at most 64 MiB of HBM per device.

```python
import math
import jax
import jax.numpy as jnp
from jax import lax

NLON = 1024
NLAT = 512
TRUNC = 341
MSLOT = 384
DSLOT = 384
MONTHS = 256


def draw_fields(key, part):
    patterns_count = 8
    half_lon = NLON // 2
    waves = jnp.arange(half_lon).astype(jnp.int32)
    longitude = jnp.arange(NLON).astype(jnp.int32)
    phase = 2.0 * math.pi * (waves[:, None] * longitude[None, :] % NLON).astype(jnp.float32) / NLON
    redness = 1.0 / (1.0 + waves.astype(jnp.float32) / (NLON / 2.0))
    cos_amps = jax.random.normal(jax.random.fold_in(key, 1), (patterns_count * NLAT, half_lon), jnp.float32) * redness
    sin_amps = jax.random.normal(jax.random.fold_in(key, 2), (patterns_count * NLAT, half_lon), jnp.float32) * redness
    patterns = jnp.dot(cos_amps, jnp.cos(phase)) + jnp.dot(sin_amps, jnp.sin(phase))
    patterns = patterns / jnp.sqrt(jnp.mean(patterns * patterns) + 1e-06)
    patterns = patterns.reshape(patterns_count, NLAT, NLON)
    month_amps = jax.random.normal(jax.random.fold_in(key, 3), (MONTHS, patterns_count), jnp.float32) / math.sqrt(patterns_count)
    month_scale = 1.0 + 2.0 * jnp.arange(MONTHS).astype(jnp.float32) / max(MONTHS - 1, 1)
    shared = jnp.einsum('tk,kjl->jtl', month_amps, patterns)
    noise = 0.5 * jax.random.normal(jax.random.fold_in(key, 4), (NLAT, MONTHS, NLON), jnp.float32)
    values = month_scale[None, :, None] * (shared + noise)
    return jnp.clip(values, -16.0, 16.0).astype(jnp.bfloat16)


def setup_inputs(seed: int = 0) -> dict:
    key_of = jax.random.split(jax.random.key(seed), 2)
    fields = draw_fields(jax.random.fold_in(key_of[1], 71), 0)
    return dict(fields=fields)


def start_value(order, sine_lat):
    log_start = 0.5 * (math.log(0.5) + lax.lgamma(order + 1.5) - (0.5 * math.log(math.pi) - math.log(2.0)) - lax.lgamma(order + 1.0)) + order * jnp.log(sine_lat)
    taper = jnp.clip((log_start + 70.0) / 10.0, 0.0, 1.0)
    return jnp.exp(jnp.maximum(log_start, -80.0)) * taper

def step_factors(order, degree):
    top = jnp.sqrt((4.0 * degree * degree - 1.0) / (degree * degree - order * order))
    below = degree - 1.0
    back = jnp.sqrt(jnp.maximum(below * below - order * order, 0.0) / jnp.abs(4.0 * below * below - 1.0))
    return (top, top * back)

def legendre_column(order, cosine_lat, sine_lat):
    first = start_value(order, sine_lat)

    def advance(carry, offset):
        current, previous = carry
        top, mixed = step_factors(order, order + offset)
        following = top * cosine_lat * current - mixed * previous
        return ((following, current), following)
    offsets = jnp.arange(1, DSLOT).astype(jnp.float32)
    _, later = lax.scan(advance, (first, jnp.zeros_like(first)), offsets)
    return jnp.concatenate([first[None, :], later], axis=0)

def weighted_basis(order, cosine_lat, sine_lat, weight):
    values = legendre_column(order, cosine_lat, sine_lat)
    offsets = jnp.arange(DSLOT).astype(jnp.float32)
    keep = (order + offsets <= TRUNC).astype(jnp.float32)
    factor = jnp.where(order > 0, math.sqrt(2.0), 1.0)
    table = values * keep[:, None] * weight[None, :] * factor
    return table.T.astype(jnp.bfloat16)

def reference(fields):
    longitude = jnp.arange(NLON).astype(jnp.int32)
    waves = jnp.arange(MSLOT).astype(jnp.int32)
    phase = 2.0 * math.pi * (longitude[:, None] * waves[None, :] % NLON).astype(jnp.float32) / NLON
    keep = (waves <= TRUNC).astype(jnp.float32)
    table = jnp.stack([jnp.cos(phase), -jnp.sin(phase)], axis=-1) * keep[None, :, None] / math.sqrt(NLON)
    table = table.reshape(NLON, 2 * MSLOT).astype(jnp.bfloat16)

    def per_row(row_fields):
        return jnp.dot(row_fields, table, preferred_element_type=jnp.float32).astype(jnp.bfloat16)
    fourier = lax.map(per_row, fields)
    fourier = fourier.reshape(NLAT, MONTHS, MSLOT, 2).transpose(2, 0, 1, 3)
    theta = math.pi * (jnp.arange(NLAT).astype(jnp.float32) + 0.5) / NLAT
    cosine_lat = jnp.cos(theta)
    sine_lat = jnp.sin(theta)
    weight = math.pi * sine_lat / NLAT

    def accumulate(gram, inputs):
        order_index, block = inputs
        order = order_index.astype(jnp.float32)
        basis = weighted_basis(order, cosine_lat, sine_lat, weight)
        coefficients = jnp.dot(block.reshape(NLAT, MONTHS * 2).T, basis, preferred_element_type=jnp.float32)
        coefficients = coefficients.astype(jnp.bfloat16).reshape(MONTHS, 2 * DSLOT)
        gram = gram + jnp.dot(coefficients, coefficients.T, preferred_element_type=jnp.float32)
        return (gram, None)
    gram, _ = lax.scan(accumulate, jnp.zeros((MONTHS, MONTHS), jnp.float32), (jnp.arange(MSLOT).astype(jnp.int32), fourier))
    trace = jnp.sum(jnp.diagonal(gram))
    return MONTHS * gram / (trace + 1e-06)
```

```python
import functools
import math

import jax
import jax.numpy as jnp
from jax import lax
from jax.experimental import pallas as pl
from jax.experimental.pallas import tpu as pltpu
from jax.sharding import PartitionSpec as P

TRUNC = 341
NLON = 1024
NLAT = 512
MONTHS = 256
OWNERS = 57
SLOTS = 6
PAIRS = 3
DEPTH = (384, 256, 128)
FIRST_ROW = (0, 384, 640)
ROWS = 768
PITCH = 60
NX = 4
NZ = 16
LATS = 64
TMS = 8
BLOCK = 8
LOCAL = 32
MESH = pl.DeviceIdType.MESH
F32 = jnp.float32
BF16 = jnp.bfloat16
SINE = tuple(
    (-1.0) ** k * (2.0 * math.pi) ** (2 * k + 1) / math.factorial(2 * k + 1) for k in range(7)
)


def sine_of_turns(u):
    square = u * u
    total = jnp.full_like(u, SINE[6])
    for k in range(5, -1, -1):
        total = total * square + SINE[k]
    return total * u


def transform_rows(step):
    pair = step // 15
    sub = lax.broadcasted_iota(jnp.int32, (16, NLON), 0)
    lon = lax.broadcasted_iota(jnp.int32, (16, NLON), 1)
    wave = (step % 15) * 4 + (sub >> 2) + OWNERS * (2 * pair + ((sub >> 1) & 1))
    phase = (wave * lon + 256 * (sub & 1)) & 1023
    away = jnp.abs(((phase + 512) & 1023) - 512)
    return sine_of_turns((256 - away).astype(F32) * (1.0 / NLON)) * (1.0 / math.sqrt(NLON))


def roll(value, shift, axis):
    return pltpu.roll(value, shift % value.shape[axis], axis)


def swap_bit(value, bit):
    rows = value.shape[0]
    sub = (lax.broadcasted_iota(jnp.int32, (rows, 128), 0) >> bit) & 1
    group = (lax.broadcasted_iota(jnp.int32, (rows, 128), 1) >> (5 + bit)) & 1
    step = 1 << bit
    from_below = roll(roll(value, 32 * step, 1), -step, 0)
    from_above = roll(roll(value, -32 * step, 1), step, 0)
    return jnp.where(sub == group, value, jnp.where(sub == 0, from_below, from_above))


def rows_by_latitude(spectrum):
    rows = spectrum.shape[0]
    low, high = spectrum[:, :128], spectrum[:, 128:]
    upper = ((lax.broadcasted_iota(jnp.int32, (rows, 128), 0) >> 2) & 1) == 0
    even = jnp.where(upper, low, roll(high, 4, 0))
    odd = jnp.where(upper, roll(low, -4, 0), high)
    return [swap_bit(swap_bit(part, 0), 1) for part in (even, odd)]


def start_value(order, sine_lat):
    ratio = jnp.ones_like(order)
    for step in range(1, 9):
        ratio = ratio * ((order + step) / (order + (step + 0.5)))
    far = order + 9.0
    inverse = 1.0 / far
    square = inverse * inverse
    series = inverse * (-1.0 / 8.0 + square * (1.0 / 192.0 - square * (1.0 / 640.0)))
    log_ratio = 0.5 * jnp.log(far) + series + jnp.log(ratio)
    constant = math.log(0.5) - (0.5 * math.log(math.pi) - math.log(2.0))
    log_start = 0.5 * (constant + log_ratio) + order * jnp.log(sine_lat)
    taper = jnp.clip((log_start + 70.0) / 10.0, 0.0, 1.0)
    return jnp.exp(jnp.maximum(log_start, -80.0)) * taper


def step_factors(order, degree):
    top = jnp.sqrt((4.0 * degree * degree - 1.0) / (degree * degree - order * order))
    below = degree - 1.0
    back = jnp.sqrt(
        jnp.maximum(below * below - order * order, 0.0) / jnp.abs(4.0 * below * below - 1.0)
    )
    return top, top * back


def legendre(owner, lane_offset):
    sub = lax.broadcasted_iota(jnp.int32, (8, 128), 0)
    order = (jnp.minimum(sub, SLOTS - 1) * OWNERS + owner).astype(F32)
    place = (lax.broadcasted_iota(jnp.int32, (8, 128), 1) + lane_offset).astype(F32) + 0.5
    turn = place * (0.5 / NLAT)
    folded = jnp.minimum(turn, 0.5 - turn)
    half = sine_of_turns(0.5 * folded)
    cosine = jnp.where(folded < 0.125, 1.0 - 2.0 * half * half, sine_of_turns(0.25 - folded))
    cosine_lat = jnp.where(turn < 0.25, cosine, -cosine)
    return order, cosine_lat, sine_of_turns(folded)


def lat_weight(width):
    turn = (lax.broadcasted_iota(jnp.int32, (1, width), 1).astype(F32) + 0.5) * (0.5 / NLAT)
    return sine_of_turns(jnp.minimum(turn, 0.5 - turn)) * (math.pi / NLAT)


def regroup(pieces):
    group = lax.broadcasted_iota(jnp.int32, (96, 128), 1) >> 5
    blocks = []
    for g in range(4):
        halves = []
        for half in range(2):
            total = None
            for a in range(4):
                moved = pieces[4 * half + a]
                if a != g:
                    moved = roll(moved, 32 * (a - g), 1)
                total = moved if total is None else jnp.where(group == a, moved, total)
            halves.append(total)
        blocks.append(jnp.concatenate(halves, axis=1))
    return jnp.concatenate(blocks, axis=0)


def owner_of(lat):
    return jnp.where(lat < 28, lat, lat - 7)


def is_owner(lat):
    return jnp.logical_or(lat < 28, lat >= 35)


def kernel(
    fields_hbm,
    out_ref,
    fields,
    transform,
    send,
    got,
    values,
    basis,
    coef,
    share,
    gram,
    slabs,
    planes,
    local_sem,
    send_sem,
    row_sem,
    month_sem,
    slab_sem,
    plane_sem,
    last_sem,
):
    lat = lax.axis_index("lat")
    tm = lax.axis_index("tm")
    z = lat // NX
    x = lat % NX
    load = pltpu.make_async_copy(fields_hbm, fields, local_sem)
    load.start()
    got[...] = jnp.zeros_like(got)

    barrier = pltpu.get_barrier_semaphore()

    def greet_lat(step, carry):
        peer = lax.rem(lat + step, LATS)
        pl.semaphore_signal(barrier, inc=1, device_id={"lat": peer}, device_id_type=MESH)
        return carry

    lax.fori_loop(1, LATS, greet_lat, 0)

    def greet_plane(step, carry):
        peer_tm = lax.rem(tm + 1 + step // NX, TMS)
        peer = z * NX + step % NX
        pl.semaphore_signal(
            barrier, inc=1, device_id={"lat": peer, "tm": peer_tm}, device_id_type=MESH
        )
        return carry

    lax.fori_loop(0, NX * (TMS - 1), greet_plane, 0)

    def fill(step, carry):
        start = pl.multiple_of(step * 16, 16)
        transform[pl.ds(start, 16), :] = transform_rows(step).astype(BF16)
        return carry

    lax.fori_loop(0, 45, fill, 0)
    load.wait()
    flat = fields[...].reshape(BLOCK * LOCAL, NLON)
    for pair in range(PAIRS):
        spectrum = lax.dot_general(
            transform[pair * 240 : (pair + 1) * 240, :],
            flat,
            (((1,), (1,)), ((), ())),
            preferred_element_type=F32,
        )
        for odd, part in enumerate(rows_by_latitude(spectrum)):
            send[:, odd, :, pair * 128 : (pair + 1) * 128] = part.reshape(
                PITCH // 2, BLOCK, 128
            ).astype(BF16)

    own = jnp.where(is_owner(lat), owner_of(lat), 400)

    @pl.when(is_owner(lat))
    def _():
        got[lat] = send[own // 2, own % 2]

    pl.semaphore_wait(barrier, LATS - 1 + NX * (TMS - 1))

    def row_copy(source, target, width):
        peer = owner_of(target)
        return pltpu.make_async_remote_copy(
            src_ref=send.at[peer // 2, peer % 2, :, pl.ds(0, width)],
            dst_ref=got.at[source, :, pl.ds(0, width)],
            send_sem=send_sem.at[0],
            recv_sem=row_sem.at[source],
            device_id={"lat": target},
            device_id_type=MESH,
        )

    near = jnp.minimum(lat, LATS - 1 - lat)
    kinds = (
        (near < 11, 128),
        (jnp.logical_and(near >= 11, near < 16), 256),
        (near >= 16, 384),
    )
    for applies, width in kinds:

        @pl.when(applies)
        def _(width=width):
            def send_both(step, carry):
                away = 32 - step

                for target in (lax.rem(lat + away, LATS), lax.rem(lat + LATS - away, LATS)):

                    @pl.when(is_owner(target))
                    def _(target=target):
                        row_copy(lat, target, width).start()

                return carry

            target = lax.rem(lat + 32, LATS)

            @pl.when(is_owner(target))
            def _():
                row_copy(lat, target, width).start()

            lax.fori_loop(1, 32, send_both, 0)

    order, _, _ = legendre(own, 0)
    cosines = []
    state = []
    for block in range(4):
        _, cosine_lat, sine_lat = legendre(own, 128 * block)
        cosines.append(cosine_lat)
        first = start_value(order, sine_lat)
        values[block, 0:8, :] = first
        state.append(first)
        state.append(jnp.zeros_like(first))

    def advance(trip, carry):
        carry = list(carry)
        for inner in range(1, 9):
            offset = trip * 8 + inner
            top, mixed = step_factors(order, order + offset.astype(F32))
            row = pl.multiple_of(offset * 8, 8)
            for block in range(4):
                current, previous = carry[2 * block], carry[2 * block + 1]
                following = top * cosines[block] * current - mixed * previous
                values[block, pl.ds(row, 8), :] = following
                carry[2 * block], carry[2 * block + 1] = following, current
        return tuple(carry)

    lax.fori_loop(0, 48, advance, tuple(state))
    weight = lat_weight(NLAT)
    for slot in range(SLOTS):
        depth = DEPTH[slot // 2]
        wave = own + OWNERS * slot
        factor = jnp.where(wave > 0, math.sqrt(2.0), 1.0).astype(F32)
        offset = lax.broadcasted_iota(jnp.int32, (depth, 128), 0)
        for block in range(4):
            lanes = slice(128 * block, 128 * (block + 1))
            table = values[block, pl.ds(slot, depth, stride=8), :]
            table = jnp.where(offset + wave <= TRUNC, table * (weight[:, lanes] * factor), 0.0)
            basis[slot, 0:depth, lanes] = table.astype(BF16)

    @pl.when(is_owner(lat))
    def _():
        for first, last, width in (
            (0, 11, 128),
            (11, 16, 256),
            (16, 48, 384),
            (48, 53, 256),
            (53, 64, 128),
        ):

            def receive(source, carry, width=width):
                @pl.when(source != lat)
                def _():
                    row_copy(source, lat, width).wait_recv()

                return carry

            lax.fori_loop(first, last, receive, 0)

    for pair in range(PAIRS):
        depth = DEPTH[pair]
        lo, hi = (16, 48) if pair == 2 else (0, 64)
        data = got[lo:hi, :, pair * 128 : (pair + 1) * 128].astype(F32)
        data = data.reshape((hi - lo) * BLOCK, 128).astype(BF16)
        both = [
            lax.dot_general(
                basis[2 * pair + side, 0:depth, lo * BLOCK : hi * BLOCK],
                data,
                (((1,), (0,)), ((), ())),
                preferred_element_type=F32,
            )
            for side in range(2)
        ]
        lane = lax.broadcasted_iota(jnp.int32, (depth, 128), 1)
        coef[FIRST_ROW[pair] : FIRST_ROW[pair] + depth, :] = jnp.where(
            lane < 64, both[0], both[1]
        ).astype(BF16)

    def month_copy(source, target):
        return pltpu.make_async_remote_copy(
            src_ref=coef.at[pl.ds(pl.multiple_of(target * 96, 96), 96), :],
            dst_ref=share.at[source],
            send_sem=send_sem.at[1],
            recv_sem=month_sem.at[source],
            device_id={"tm": target},
            device_id_type=MESH,
        )

    for step in range(1, TMS):
        month_copy(tm, lax.rem(tm + step, TMS)).start()
    share[tm] = coef[pl.ds(pl.multiple_of(tm * 96, 96), 96), :]
    for step in range(1, TMS):
        month_copy(lax.rem(tm + step, TMS), tm).wait_recv()
    columns = regroup([share[source].astype(F32) for source in range(TMS)]).astype(BF16)
    terms = lax.dot_general(
        columns, columns, (((0,), (0,)), ((), ())), preferred_element_type=F32
    )
    row = lax.broadcasted_iota(jnp.int32, (MONTHS, MONTHS), 0)
    col = lax.broadcasted_iota(jnp.int32, (MONTHS, MONTHS), 1)
    diagonal = jnp.where(row == col, terms, 0.0)
    trace = jnp.sum(jnp.sum(diagonal, axis=0, keepdims=True), axis=1, keepdims=True)
    spare = jnp.logical_and((row & 7) == 1, col == row - 1)
    gram[...] = jnp.where(spare, trace, terms).reshape(32, 8, MONTHS)

    def slab_copy(source, target_x, target_tm):
        return pltpu.make_async_remote_copy(
            src_ref=gram.at[target_tm * NX + target_x],
            dst_ref=slabs.at[source],
            send_sem=send_sem.at[2],
            recv_sem=slab_sem.at[source],
            device_id={"lat": z * NX + target_x, "tm": target_tm},
            device_id_type=MESH,
        )

    me = tm * NX + x

    def send_slab(step, carry):
        target = lax.rem(me + step, 32)
        slab_copy(me, target % NX, target // NX).start()
        return carry

    lax.fori_loop(1, 32, send_slab, 0)
    slabs[me] = gram[me]

    def receive_slab(step, carry):
        slab_copy(lax.rem(me + step, 32), x, tm).wait_recv()
        return carry

    lax.fori_loop(1, 32, receive_slab, 0)
    planes[z] = jnp.sum(slabs[...], axis=0)

    def plane_copy(source, target):
        return pltpu.make_async_remote_copy(
            src_ref=planes.at[z],
            dst_ref=planes.at[source],
            send_sem=send_sem.at[3],
            recv_sem=plane_sem.at[source],
            device_id={"lat": target * NX + x},
            device_id_type=MESH,
        )

    for away in (8, 7, 9, 6, 10, 5, 11, 4, 12, 3, 13, 2, 14, 1, 15):
        plane_copy(z, lax.rem(z + away, NZ)).start()
    for away in range(1, NZ):
        plane_copy(lax.rem(z + away, NZ), z).wait_recv()
    slab = jnp.sum(planes[...], axis=0)
    row = lax.broadcasted_iota(jnp.int32, (BLOCK, MONTHS), 0)
    col = lax.broadcasted_iota(jnp.int32, (BLOCK, MONTHS), 1) - 8 * me
    spare = jnp.logical_and(row == 1, col == 0)
    twin = jnp.logical_and(row == 0, col == 1)

    def pick(mask):
        chosen = jnp.sum(jnp.where(mask, slab, 0.0), axis=0, keepdims=True)
        return jnp.sum(chosen, axis=1, keepdims=True)

    total = pick(spare)
    out_ref[x] = jnp.where(spare, pick(twin), slab) * (MONTHS / (total + 1e-06))

    def last_copy(source, target):
        return pltpu.make_async_remote_copy(
            src_ref=out_ref.at[source],
            dst_ref=out_ref.at[source],
            send_sem=send_sem.at[4],
            recv_sem=last_sem.at[source],
            device_id={"lat": z * NX + target},
            device_id_type=MESH,
        )

    for away in (2, 1, 3):
        last_copy(x, lax.rem(x + away, NX)).start()
    for away in range(1, NX):
        last_copy(lax.rem(x + away, NX), x).wait_recv()

    for applies, width in kinds:

        @pl.when(applies)
        def _(width=width):
            def sent(step, carry):
                target = lax.rem(lat + step, LATS)

                @pl.when(is_owner(target))
                def _():
                    row_copy(lat, target, width).wait_send()

                return carry

            lax.fori_loop(1, LATS, sent, 0)

    for step in range(1, TMS):
        month_copy(tm, lax.rem(tm + step, TMS)).wait_send()

    def slab_sent(step, carry):
        target = lax.rem(me + step, 32)
        slab_copy(me, target % NX, target // NX).wait_send()
        return carry

    lax.fori_loop(1, 32, slab_sent, 0)
    for away in range(1, NZ):
        plane_copy(z, lax.rem(z + away, NZ)).wait_send()
    for away in range(1, NX):
        last_copy(x, lax.rem(x + away, NX)).wait_send()


def local(fields):
    call = pl.pallas_call(
        kernel,
        out_shape=jax.ShapeDtypeStruct((NX, BLOCK, MONTHS), F32),
        in_specs=[pl.BlockSpec(memory_space=pl.ANY)],
        out_specs=pl.BlockSpec(memory_space=pltpu.VMEM),
        scratch_shapes=[
            pltpu.VMEM((BLOCK, LOCAL, NLON), BF16),
            pltpu.VMEM((PAIRS * 240, NLON), BF16),
            pltpu.VMEM((PITCH // 2, 2, BLOCK, 384), BF16),
            pltpu.VMEM((LATS, BLOCK, 384), BF16),
            pltpu.VMEM((4, 385 * 8, 128), F32),
            pltpu.VMEM((SLOTS, 384, NLAT), BF16),
            pltpu.VMEM((ROWS, 128), BF16),
            pltpu.VMEM((TMS, 96, 128), BF16),
            pltpu.VMEM((32, BLOCK, MONTHS), F32),
            pltpu.VMEM((32, BLOCK, MONTHS), F32),
            pltpu.VMEM((NZ, BLOCK, MONTHS), F32),
            pltpu.SemaphoreType.DMA,
            pltpu.SemaphoreType.DMA((5,)),
            pltpu.SemaphoreType.DMA((LATS,)),
            pltpu.SemaphoreType.DMA((TMS,)),
            pltpu.SemaphoreType.DMA((32,)),
            pltpu.SemaphoreType.DMA((NZ,)),
            pltpu.SemaphoreType.DMA((NX,)),
        ],
        compiler_params=pltpu.CompilerParams(
            collective_id=0, has_side_effects=True, vmem_limit_bytes=48 * 1024 * 1024
        ),
    )
    return call(fields).reshape(LOCAL, MONTHS)


def solution(mesh):
    return jax.shard_map(
        local,
        mesh=mesh,
        in_specs=(P("lat", "tm", None),),
        out_specs=P("tm", None),
        check_vma=False,
    )
```

```python
import functools
import math

import jax
import jax.numpy as jnp
from jax import lax
from jax.experimental import pallas as pl
from jax.experimental.pallas import tpu as pltpu
from jax.sharding import PartitionSpec as P

TRUNC = 341
NLON = 1024
NLAT = 512
MONTHS = 256
LATS = 64
TMS = 8
NX = 4
BLOCK = 8
LOCAL = 32
MIDDLE = 21
INNER = 22
OUTER = 42
DEPTH_OUT = (352, 272)
DEPTH_IN = (176, 144, 96, 48)
ROWS = 640
PART = ROWS // TMS
PITCH_OUT = 44
PITCH_IN = 24
KINDS = (
    (0, 9, 128, 0),
    (9, 14, 256, 0),
    (14, 16, 256, 128),
    (16, 17, 256, 256),
    (17, 18, 256, 384),
    (18, 32, 256, 512),
)
MESH = pl.DeviceIdType.MESH
F32 = jnp.float32
BF16 = jnp.bfloat16
SINE = tuple(
    (-1.0) ** k * (2.0 * math.pi) ** (2 * k + 1) / math.factorial(2 * k + 1) for k in range(7)
)


def sine_of_turns(u):
    square = u * u
    total = jnp.full_like(u, SINE[6])
    for k in range(5, -1, -1):
        total = total * square + SINE[k]
    return total * u


def cosine_of_phase(phase):
    away = jnp.abs(((phase + 512) & 1023) - 512)
    return sine_of_turns((256 - away).astype(F32) * (1.0 / NLON))


def waves_times_lon(first, slot_step, owner_step, part_step):
    sub = lax.broadcasted_iota(jnp.int32, (8, NLON), 0)
    lon = lax.broadcasted_iota(jnp.int32, (8, NLON), 1)
    wave = first + slot_step * ((sub >> 1) & 1) + owner_step * (sub >> 2)
    return wave * lon + part_step * (sub & 1)


def cosine_sine(phase):
    return cosine_of_phase(phase), cosine_of_phase(phase - 256)


def turn(pair, by):
    cosine, sine = pair
    return cosine * by[0] - sine * by[1], sine * by[0] + cosine * by[1]


def roll(value, shift, axis):
    return pltpu.roll(value, shift % value.shape[axis], axis)


def swap_bit(value, bit):
    rows = value.shape[0]
    sub = (lax.broadcasted_iota(jnp.int32, (rows, 128), 0) >> bit) & 1
    group = (lax.broadcasted_iota(jnp.int32, (rows, 128), 1) >> (5 + bit)) & 1
    step = 1 << bit
    from_below = roll(roll(value, 32 * step, 1), -step, 0)
    from_above = roll(roll(value, -32 * step, 1), step, 0)
    return jnp.where(sub == group, value, jnp.where(sub == 0, from_below, from_above))


def rows_by_latitude(spectrum):
    low, high = spectrum[:, :128], spectrum[:, 128:]
    return [swap_bit(swap_bit(part, 0), 1) for part in exchange_halves(low, high)]


def start_value(order, sine_lat):
    ratio = jnp.ones_like(order)
    for step in range(1, 9):
        ratio = ratio * ((order + step) / (order + (step + 0.5)))
    far = order + 9.0
    inverse = 1.0 / far
    square = inverse * inverse
    series = inverse * (-1.0 / 8.0 + square * (1.0 / 192.0 - square * (1.0 / 640.0)))
    log_ratio = 0.5 * jnp.log(far) + series + jnp.log(ratio)
    constant = math.log(0.5) - (0.5 * math.log(math.pi) - math.log(2.0))
    log_start = 0.5 * (constant + log_ratio) + order * jnp.log(sine_lat)
    taper = jnp.clip((log_start + 70.0) / 10.0, 0.0, 1.0)
    return jnp.exp(jnp.maximum(log_start, -80.0)) * taper


def step_factors(order, degree):
    top = jnp.sqrt((4.0 * degree * degree - 1.0) / (degree * degree - order * order))
    below = degree - 1.0
    back = jnp.sqrt(
        jnp.maximum(below * below - order * order, 0.0) / jnp.abs(4.0 * below * below - 1.0)
    )
    return top, top * back


def legendre(waves, lane_offset):
    place = (lax.broadcasted_iota(jnp.int32, (8, 128), 1) + lane_offset).astype(F32) + 0.5
    turns = place * (0.5 / NLAT)
    folded = jnp.minimum(turns, 0.5 - turns)
    half = sine_of_turns(0.5 * folded)
    cosine = jnp.where(folded < 0.125, 1.0 - 2.0 * half * half, sine_of_turns(0.25 - folded))
    return jnp.where(turns < 0.25, cosine, -cosine), sine_of_turns(folded)


def lat_weight(width):
    turns = (lax.broadcasted_iota(jnp.int32, (1, width), 1).astype(F32) + 0.5) * (0.5 / NLAT)
    return sine_of_turns(jnp.minimum(turns, 0.5 - turns)) * (math.pi / NLAT)


def regroup(pieces):
    group = lax.broadcasted_iota(jnp.int32, (PART, 128), 1) >> 5
    blocks = []
    for g in range(4):
        halves = []
        for half in range(2):
            total = None
            for a in range(4):
                moved = pieces[4 * half + a]
                if a != g:
                    moved = roll(moved, 32 * (a - g), 1)
                total = moved if total is None else jnp.where(group == a, moved, total)
            halves.append(total)
        blocks.append(jnp.concatenate(halves, axis=1))
    return jnp.concatenate(blocks, axis=0)


def exchange_halves(left, right):
    upper = ((lax.broadcasted_iota(jnp.int32, left.shape, 0) >> 2) & 1) == 0
    return (
        jnp.where(upper, left, roll(right, 4, 0)),
        jnp.where(upper, roll(left, -4, 0), right),
    )


def wrapped(value, length):
    return jnp.where(value >= length, value - length, value)


def is_inner(lat):
    return jnp.logical_and(lat >= MIDDLE, lat < MIDDLE + INNER)


def outer_owner(lat):
    return jnp.where(lat < MIDDLE, lat, lat - INNER)


def kernel(
    fields_hbm,
    out_ref,
    fields,
    patterns,
    transform,
    send_out,
    send_in,
    got,
    values,
    basis,
    coef,
    share,
    gram,
    slabs,
    planes,
    finals,
    local_sem,
    send_sem,
    row_sem,
    month_sem,
    slab_sem,
    plane_sem,
    last_sem,
):
    lat = lax.axis_index("lat")
    tm = lax.axis_index("tm")
    z = lat // NX
    x = lat % NX
    half = z % 2
    inner = is_inner(lat)
    outer = jnp.logical_not(inner)
    load = pltpu.make_async_copy(fields_hbm, fields, local_sem)
    load.start()
    got[...] = jnp.zeros_like(got)

    barrier = pltpu.get_barrier_semaphore()
    for away in range(32, 0, -1):
        for step in {away, LATS - away}:
            pl.semaphore_signal(
                barrier,
                inc=1,
                device_id={"lat": wrapped(lat + step, LATS)},
                device_id_type=MESH,
            )
    for step in range(1, TMS):
        pl.semaphore_signal(
            barrier, inc=1, device_id={"tm": wrapped(tm + step, TMS)}, device_id_type=MESH
        )

    for index in range(6):
        if index < 2:
            phase = waves_times_lon(2 * OUTER * index, OUTER, 0, 256)
        else:
            phase = waves_times_lon(168 + 2 * INNER * (index - 2), INNER, 0, 256)
        cosine, sine = cosine_sine(phase)
        patterns[2 * index] = cosine * (1.0 / math.sqrt(NLON))
        patterns[2 * index + 1] = sine * (1.0 / math.sqrt(NLON))
    by = cosine_sine(waves_times_lon(2, 0, 0, 0))

    def fill(kinds, trip, pair):
        following = turn(pair, by)
        for index in kinds:
            first = 176 * index if index < 2 else 352 + 96 * (index - 2)
            rows = [
                cosine * patterns[2 * index] - sine * patterns[2 * index + 1]
                for cosine, sine in (pair, following)
            ]
            start = pl.multiple_of(first + trip * 16, 16)
            transform[pl.ds(start, 16), :] = jnp.concatenate(rows, axis=0).astype(BF16)
        return turn(following, by)

    pair = cosine_sine(waves_times_lon(0, 0, 1, 0))
    pair = lax.fori_loop(0, 6, functools.partial(fill, range(6)), pair)
    lax.fori_loop(6, 11, functools.partial(fill, range(2)), pair)
    load.wait()
    flat = fields[...].reshape(BLOCK * LOCAL, NLON)
    for index in range(6):
        first, rows, buffer, place = (
            (176 * index, 176, send_out, index)
            if index < 2
            else (352 + 96 * (index - 2), 96, send_in, index - 2)
        )
        spectrum = lax.dot_general(
            transform[first : first + rows, :],
            flat,
            (((1,), (1,)), ((), ())),
            preferred_element_type=F32,
        )
        for odd, part in enumerate(rows_by_latitude(spectrum)):
            buffer[:, odd, :, place * 128 : (place + 1) * 128] = part.reshape(
                rows // 8, BLOCK, 128
            ).astype(BF16)

    own = jnp.where(inner, lat - MIDDLE, outer_owner(lat))

    @pl.when(inner)
    def _():
        got[lat] = send_in[own // 2, own % 2]

    @pl.when(outer)
    def _():
        got[lat, :, 0:256] = send_out[own // 2, own % 2]

    pl.semaphore_wait(barrier, LATS - 1 + TMS - 1)

    def row_copy(source, target, width, to_inner):
        if to_inner:
            peer = target - MIDDLE
            buffer = send_in
        else:
            peer = outer_owner(target)
            buffer = send_out
        return pltpu.make_async_remote_copy(
            src_ref=buffer.at[peer // 2, peer % 2, :, pl.ds(0, width)],
            dst_ref=got.at[source, :, pl.ds(0, width)],
            send_sem=send_sem.at[0],
            recv_sem=row_sem.at[source],
            device_id={"lat": target},
            device_id_type=MESH,
        )

    near = jnp.minimum(lat, LATS - 1 - lat)

    def each_row_copy(action):
        for lo, hi, width_out, width_in in KINDS:

            @pl.when(jnp.logical_and(near >= lo, near < hi))
            def _(width_out=width_out, width_in=width_in):
                def one(target):
                    to_inner = is_inner(target)

                    @pl.when(jnp.logical_not(to_inner))
                    def _():
                        action(row_copy(lat, target, width_out, False))

                    if width_in:

                        @pl.when(to_inner)
                        def _():
                            action(row_copy(lat, target, width_in, True))

                def both(step, carry):
                    one(wrapped(lat + (32 - step), LATS))
                    one(wrapped(lat + (32 + step), LATS))
                    return carry

                one(wrapped(lat + 32, LATS))
                lax.fori_loop(1, 32, both, 0)

    each_row_copy(lambda copy: copy.start())

    base = jnp.where(inner, 168, 0) + own
    stride = jnp.where(inner, INNER, OUTER)
    slot = jnp.minimum(
        lax.broadcasted_iota(jnp.int32, (8, 128), 0), jnp.where(inner, 7, 3)
    )
    order = (base + stride * slot).astype(F32)
    cosines = []
    state = []
    for block in range(4):
        cosine_lat, sine_lat = legendre(order, 128 * block)
        cosines.append(cosine_lat)
        first = start_value(order, sine_lat)
        values[block, 0:8, :] = first
        state.append(first)
        state.append(jnp.zeros_like(first))

    def advance(trip, carry):
        carry = list(carry)
        for step in range(1, 9):
            offset = trip * 8 + step
            top, mixed = step_factors(order, order + offset.astype(F32))
            row = pl.multiple_of(offset * 8, 8)
            for block in range(4):
                current, previous = carry[2 * block], carry[2 * block + 1]
                following = top * cosines[block] * current - mixed * previous
                values[block, pl.ds(row, 8), :] = following
                carry[2 * block], carry[2 * block + 1] = following, current
        return tuple(carry)

    lax.fori_loop(0, 44, advance, tuple(state))
    weight = lat_weight(NLAT)

    def tabulate(depths):
        for slot in range(2 * len(depths)):
            depth = depths[slot // 2]
            wave = base + stride * slot
            factor = jnp.where(wave > 0, math.sqrt(2.0), 1.0).astype(F32)
            offset = lax.broadcasted_iota(jnp.int32, (depth, 128), 0)
            for block in range(4):
                lanes = slice(128 * block, 128 * (block + 1))
                table = values[block, pl.ds(slot, depth, stride=8), :]
                table = jnp.where(
                    offset + wave <= TRUNC, table * (weight[:, lanes] * factor), 0.0
                )
                basis[slot, 0:depth, lanes] = table.astype(BF16)

    def receive(to_inner):
        for lo, hi, width_out, width_in in KINDS:
            width = width_in if to_inner else width_out
            if width:

                def one(source, carry, width=width):
                    @pl.when(source != lat)
                    def _():
                        row_copy(source, lat, width, to_inner).wait_recv()

                    return carry

                lax.fori_loop(lo, hi, one, 0)
                lax.fori_loop(LATS - hi, LATS - lo, one, 0)

    def combine(depths, narrow_from):
        first = 0
        for pair, depth in enumerate(depths):
            lo, hi = (16, 48) if pair >= narrow_from else (0, 64)
            data = got[lo:hi, :, pair * 128 : (pair + 1) * 128].astype(F32)
            data = data.reshape((hi - lo) * BLOCK, 128).astype(BF16)
            both = [
                lax.dot_general(
                    basis[2 * pair + side, 0:depth, lo * BLOCK : hi * BLOCK],
                    data,
                    (((1,), (0,)), ((), ())),
                    preferred_element_type=F32,
                )
                for side in range(2)
            ]
            lane = lax.broadcasted_iota(jnp.int32, (depth, 128), 1)
            coef[first : first + depth, :] = jnp.where(lane < 64, both[0], both[1]).astype(BF16)
            first += depth
        coef[first:ROWS, :] = jnp.zeros((ROWS - first, 128), BF16)

    @pl.when(outer)
    def _():
        tabulate(DEPTH_OUT)
        receive(False)
        combine(DEPTH_OUT, 2)

    @pl.when(inner)
    def _():
        tabulate(DEPTH_IN)
        receive(True)
        combine(DEPTH_IN, 2)

    def month_copy(source, target):
        return pltpu.make_async_remote_copy(
            src_ref=coef.at[pl.ds(pl.multiple_of(target * PART, PART), PART), :],
            dst_ref=share.at[source],
            send_sem=send_sem.at[1],
            recv_sem=month_sem.at[source],
            device_id={"tm": target},
            device_id_type=MESH,
        )

    for step in range(1, TMS):
        month_copy(tm, wrapped(tm + step, TMS)).start()
    share[tm] = coef[pl.ds(pl.multiple_of(tm * PART, PART), PART), :]
    for step in range(1, TMS):
        month_copy(wrapped(tm + step, TMS), tm).wait_recv()
    columns = regroup([share[source].astype(F32) for source in range(TMS)]).astype(BF16)
    terms = lax.dot_general(
        columns, columns, (((0,), (0,)), ((), ())), preferred_element_type=F32
    )
    row = lax.broadcasted_iota(jnp.int32, (MONTHS, MONTHS), 0)
    col = lax.broadcasted_iota(jnp.int32, (MONTHS, MONTHS), 1)
    diagonal = jnp.where(row == col, terms, 0.0)
    trace = jnp.sum(jnp.sum(diagonal, axis=0, keepdims=True), axis=1, keepdims=True)
    spare = jnp.logical_and((row & 3) == 1, col == row - 1)
    terms = jnp.where(spare, trace, terms)
    for odd, part in enumerate(exchange_halves(terms[:, :128], terms[:, 128:])):
        gram[:, odd] = part.reshape(32, 8, 128)

    me = tm * 8 + x * 2 + half

    def slab_copy(source, target):
        place = target % 8
        return pltpu.make_async_remote_copy(
            src_ref=gram.at[target // 2, target % 2],
            dst_ref=slabs.at[source],
            send_sem=send_sem.at[2],
            recv_sem=slab_sem.at[source],
            device_id={"lat": (z - half + place % 2) * NX + place // 2, "tm": target // 8},
            device_id_type=MESH,
        )

    def send_slab(step, carry):
        slab_copy(me, wrapped(me + step, 64)).start()
        return carry

    lax.fori_loop(1, 64, send_slab, 0)
    slabs[me] = gram[me // 2, me % 2]

    def receive_slab(step, carry):
        slab_copy(wrapped(me + step, 64), me).wait_recv()
        return carry

    lax.fori_loop(1, 64, receive_slab, 0)
    own_pair = z // 2
    planes[own_pair] = jnp.sum(slabs[...], axis=0)

    def plane_copy(source, target):
        return pltpu.make_async_remote_copy(
            src_ref=planes.at[own_pair],
            dst_ref=planes.at[source],
            send_sem=send_sem.at[3],
            recv_sem=plane_sem.at[source],
            device_id={"lat": (target * 2 + half) * NX + x},
            device_id_type=MESH,
        )

    for away in (4, 3, 5, 2, 6, 1, 7):
        plane_copy(own_pair, wrapped(own_pair + away, 8)).start()

    each_row_copy(lambda copy: copy.wait_send())
    for step in range(1, TMS):
        month_copy(tm, wrapped(tm + step, TMS)).wait_send()

    def slab_sent(step, carry):
        slab_copy(me, wrapped(me + step, 64)).wait_send()
        return carry

    lax.fori_loop(1, 64, slab_sent, 0)

    for away in range(1, 8):
        plane_copy(wrapped(own_pair + away, 8), own_pair).wait_recv()
    slab = jnp.sum(planes[...], axis=0)
    later = me // 32
    row = lax.broadcasted_iota(jnp.int32, (8, 128), 0) - 4 * later
    col = lax.broadcasted_iota(jnp.int32, (8, 128), 1) - (4 * me - 128 * later)
    spare = jnp.logical_and(row == 1, col == 0)
    twin = jnp.logical_and(row == 0, col == 1)

    def pick(mask):
        chosen = jnp.sum(jnp.where(mask, slab, 0.0), axis=0, keepdims=True)
        return jnp.sum(chosen, axis=1, keepdims=True)

    total = pick(spare)
    place = x * 2 + half
    finals[place] = jnp.where(spare, pick(twin), slab) * (MONTHS / (total + 1e-06))

    def last_copy(source, target):
        return pltpu.make_async_remote_copy(
            src_ref=finals.at[place],
            dst_ref=finals.at[source],
            send_sem=send_sem.at[4],
            recv_sem=last_sem.at[source],
            device_id={"lat": (z - half + target % 2) * NX + target // 2},
            device_id_type=MESH,
        )

    for away in (4, 5, 3, 2, 6, 1, 7):
        last_copy(place, wrapped(place + away, 8)).start()
    for away in range(1, 8):
        plane_copy(own_pair, wrapped(own_pair + away, 8)).wait_send()
    for away in range(1, 8):
        last_copy(wrapped(place + away, 8), place).wait_recv()
    for index in range(4):
        left, right = exchange_halves(finals[2 * index], finals[2 * index + 1])
        out_ref[8 * index : 8 * (index + 1), 0:128] = left
        out_ref[8 * index : 8 * (index + 1), 128:256] = right
    for away in range(1, 8):
        last_copy(place, wrapped(place + away, 8)).wait_send()


def local(fields):
    return pl.pallas_call(
        kernel,
        out_shape=jax.ShapeDtypeStruct((LOCAL, MONTHS), F32),
        in_specs=[pl.BlockSpec(memory_space=pltpu.HBM)],
        out_specs=pl.BlockSpec(memory_space=pltpu.VMEM),
        scratch_shapes=[
            pltpu.VMEM((BLOCK, LOCAL, NLON), BF16),
            pltpu.VMEM((12, 8, NLON), F32),
            pltpu.VMEM((736, NLON), BF16),
            pltpu.VMEM((PITCH_OUT // 2, 2, BLOCK, 256), BF16),
            pltpu.VMEM((PITCH_IN // 2, 2, BLOCK, 512), BF16),
            pltpu.VMEM((LATS, BLOCK, 512), BF16),
            pltpu.VMEM((4, 353 * 8, 128), F32),
            pltpu.VMEM((8, 352, NLAT), BF16),
            pltpu.VMEM((ROWS, 128), BF16),
            pltpu.VMEM((TMS, PART, 128), BF16),
            pltpu.VMEM((32, 2, 8, 128), F32),
            pltpu.VMEM((64, 8, 128), F32),
            pltpu.VMEM((8, 8, 128), F32),
            pltpu.VMEM((8, 8, 128), F32),
            pltpu.SemaphoreType.DMA,
            pltpu.SemaphoreType.DMA((5,)),
            pltpu.SemaphoreType.DMA((LATS,)),
            pltpu.SemaphoreType.DMA((TMS,)),
            pltpu.SemaphoreType.DMA((64,)),
            pltpu.SemaphoreType.DMA((8,)),
            pltpu.SemaphoreType.DMA((8,)),
        ],
        compiler_params=pltpu.CompilerParams(
            collective_id=0, has_side_effects=True, vmem_limit_bytes=67_043_328
        ),
    )(fields)


def solution(mesh):
    return jax.shard_map(
        local,
        mesh=mesh,
        in_specs=(P("lat", "tm", None),),
        out_specs=P("tm", None),
        check_vma=False,
    )
```

```python
import functools
import math

import jax
import jax.numpy as jnp
from jax import lax
from jax.experimental import pallas as pl
from jax.experimental.pallas import tpu as pltpu
from jax.sharding import PartitionSpec as P

TRUNC = 341
NLON = 1024
NLAT = 512
MONTHS = 256
LATS = 64
TMS = 8
NX = 4
BLOCK = 8
LOCAL = 32
MIDDLE = 21
INNER = 22
OUTER = 42
DEPTH_OUT = (352, 272)
DEPTH_IN = (176, 144, 96, 48)
PART_OUT = 80
PART_IN = 64
PITCH_OUT = 44
PITCH_IN = 24
KINDS = (
    (0, 9, 128, 0),
    (9, 14, 256, 0),
    (14, 16, 256, 128),
    (16, 17, 256, 256),
    (17, 18, 256, 384),
    (18, 32, 256, 512),
)
MESH = pl.DeviceIdType.MESH
F32 = jnp.float32
BF16 = jnp.bfloat16
SINE = tuple(
    (-1.0) ** k * (2.0 * math.pi) ** (2 * k + 1) / math.factorial(2 * k + 1) for k in range(7)
)


def sine_of_turns(u):
    square = u * u
    total = jnp.full_like(u, SINE[6])
    for k in range(5, -1, -1):
        total = total * square + SINE[k]
    return total * u


def cosine_of_phase(phase):
    away = jnp.abs(((phase + 512) & 1023) - 512)
    return sine_of_turns((256 - away).astype(F32) * (1.0 / NLON))


def waves_times_lon(first, slot_step, owner_step, part_step):
    sub = lax.broadcasted_iota(jnp.int32, (8, NLON), 0)
    lon = lax.broadcasted_iota(jnp.int32, (8, NLON), 1)
    wave = first + slot_step * ((sub >> 1) & 1) + owner_step * (sub >> 2)
    return wave * lon + part_step * (sub & 1)


def cosine_sine(phase):
    return cosine_of_phase(phase), cosine_of_phase(phase - 256)


def turn(pair, by):
    cosine, sine = pair
    return cosine * by[0] - sine * by[1], sine * by[0] + cosine * by[1]


def roll(value, shift, axis):
    return pltpu.roll(value, shift % value.shape[axis], axis)


def swap_bit(value, bit):
    rows = value.shape[0]
    sub = (lax.broadcasted_iota(jnp.int32, (rows, 128), 0) >> bit) & 1
    group = (lax.broadcasted_iota(jnp.int32, (rows, 128), 1) >> (5 + bit)) & 1
    step = 1 << bit
    from_below = roll(roll(value, 32 * step, 1), -step, 0)
    from_above = roll(roll(value, -32 * step, 1), step, 0)
    return jnp.where(sub == group, value, jnp.where(sub == 0, from_below, from_above))


def rows_by_latitude(spectrum):
    low, high = spectrum[:, :128], spectrum[:, 128:]
    return [swap_bit(swap_bit(part, 0), 1) for part in exchange_halves(low, high)]


def start_value(order, sine_lat):
    ratio = jnp.ones_like(order)
    for step in range(1, 9):
        ratio = ratio * ((order + step) / (order + (step + 0.5)))
    far = order + 9.0
    inverse = 1.0 / far
    square = inverse * inverse
    series = inverse * (-1.0 / 8.0 + square * (1.0 / 192.0 - square * (1.0 / 640.0)))
    log_ratio = 0.5 * jnp.log(far) + series + jnp.log(ratio)
    constant = math.log(0.5) - (0.5 * math.log(math.pi) - math.log(2.0))
    log_start = 0.5 * (constant + log_ratio) + order * jnp.log(sine_lat)
    taper = jnp.clip((log_start + 70.0) / 10.0, 0.0, 1.0)
    return jnp.exp(jnp.maximum(log_start, -80.0)) * taper


def step_factors(order, degree):
    top = jnp.sqrt((4.0 * degree * degree - 1.0) / (degree * degree - order * order))
    below = degree - 1.0
    back = jnp.sqrt(
        jnp.maximum(below * below - order * order, 0.0) / jnp.abs(4.0 * below * below - 1.0)
    )
    return top, top * back


def legendre(waves, lane_offset):
    place = (lax.broadcasted_iota(jnp.int32, (8, 128), 1) + lane_offset).astype(F32) + 0.5
    turns = place * (0.5 / NLAT)
    folded = jnp.minimum(turns, 0.5 - turns)
    half = sine_of_turns(0.5 * folded)
    cosine = jnp.where(folded < 0.125, 1.0 - 2.0 * half * half, sine_of_turns(0.25 - folded))
    return jnp.where(turns < 0.25, cosine, -cosine), sine_of_turns(folded)


def lat_weight(width):
    turns = (lax.broadcasted_iota(jnp.int32, (1, width), 1).astype(F32) + 0.5) * (0.5 / NLAT)
    return sine_of_turns(jnp.minimum(turns, 0.5 - turns)) * (math.pi / NLAT)


def regroup(pieces):
    group = lax.broadcasted_iota(jnp.int32, pieces[0].shape, 1) >> 5
    blocks = []
    for g in range(4):
        halves = []
        for half in range(2):
            total = None
            for a in range(4):
                moved = pieces[4 * half + a]
                if a != g:
                    moved = roll(moved, 32 * (a - g), 1)
                total = moved if total is None else jnp.where(group == a, moved, total)
            halves.append(total)
        blocks.append(jnp.concatenate(halves, axis=1))
    return jnp.concatenate(blocks, axis=0)


def exchange_halves(left, right):
    upper = ((lax.broadcasted_iota(jnp.int32, left.shape, 0) >> 2) & 1) == 0
    return (
        jnp.where(upper, left, roll(right, 4, 0)),
        jnp.where(upper, roll(left, -4, 0), right),
    )


def wrapped(value, length):
    return jnp.where(value >= length, value - length, value)


def is_inner(lat):
    return jnp.logical_and(lat >= MIDDLE, lat < MIDDLE + INNER)


def outer_owner(lat):
    return jnp.where(lat < MIDDLE, lat, lat - INNER)


def kernel(
    fields_hbm,
    out_ref,
    fields,
    patterns,
    transform,
    send_out,
    send_in,
    got,
    values,
    basis,
    coef,
    share,
    gram,
    slabs,
    planes,
    finals,
    local_sem,
    send_sem,
    row_sem,
    month_sem,
    slab_sem,
    plane_sem,
    last_sem,
):
    lat = lax.axis_index("lat")
    tm = lax.axis_index("tm")
    z = lat // NX
    x = lat % NX
    half = z % 2
    inner = is_inner(lat)
    outer = jnp.logical_not(inner)
    load = pltpu.make_async_copy(fields_hbm, fields, local_sem)
    load.start()
    got[...] = jnp.zeros_like(got)

    barrier = pltpu.get_barrier_semaphore()
    for away in range(32, 0, -1):
        for step in {away, LATS - away}:
            pl.semaphore_signal(
                barrier,
                inc=1,
                device_id={"lat": wrapped(lat + step, LATS)},
                device_id_type=MESH,
            )
    for step in range(1, TMS):
        pl.semaphore_signal(
            barrier, inc=1, device_id={"tm": wrapped(tm + step, TMS)}, device_id_type=MESH
        )

    for index in range(6):
        if index < 2:
            phase = waves_times_lon(2 * OUTER * index, OUTER, 0, 256)
        else:
            phase = waves_times_lon(168 + 2 * INNER * (index - 2), INNER, 0, 256)
        cosine, sine = cosine_sine(phase)
        patterns[2 * index] = cosine * (1.0 / math.sqrt(NLON))
        patterns[2 * index + 1] = sine * (1.0 / math.sqrt(NLON))
    by = cosine_sine(waves_times_lon(2, 0, 0, 0))

    def fill(kinds, trip, pair):
        following = turn(pair, by)
        for index in kinds:
            first = 176 * index if index < 2 else 352 + 96 * (index - 2)
            rows = [
                cosine * patterns[2 * index] - sine * patterns[2 * index + 1]
                for cosine, sine in (pair, following)
            ]
            start = pl.multiple_of(first + trip * 16, 16)
            transform[pl.ds(start, 16), :] = jnp.concatenate(rows, axis=0).astype(BF16)
        return turn(following, by)

    pair = cosine_sine(waves_times_lon(0, 0, 1, 0))
    pair = lax.fori_loop(0, 6, functools.partial(fill, range(6)), pair)
    lax.fori_loop(6, 11, functools.partial(fill, range(2)), pair)
    load.wait()
    flat = fields[...].reshape(BLOCK * LOCAL, NLON)
    for index in range(6):
        first, rows, buffer, place = (
            (176 * index, 176, send_out, index)
            if index < 2
            else (352 + 96 * (index - 2), 96, send_in, index - 2)
        )
        spectrum = lax.dot_general(
            transform[first : first + rows, :],
            flat,
            (((1,), (1,)), ((), ())),
            preferred_element_type=F32,
        )
        for odd, part in enumerate(rows_by_latitude(spectrum)):
            buffer[:, odd, :, place * 128 : (place + 1) * 128] = part.reshape(
                rows // 8, BLOCK, 128
            ).astype(BF16)

    own = jnp.where(inner, lat - MIDDLE, outer_owner(lat))

    @pl.when(inner)
    def _():
        got[lat] = send_in[own // 2, own % 2]

    @pl.when(outer)
    def _():
        got[lat, :, 0:256] = send_out[own // 2, own % 2]

    pl.semaphore_wait(barrier, LATS - 1 + TMS - 1)

    def row_copy(source, target, width, to_inner):
        if to_inner:
            peer = target - MIDDLE
            buffer = send_in
        else:
            peer = outer_owner(target)
            buffer = send_out
        return pltpu.make_async_remote_copy(
            src_ref=buffer.at[peer // 2, peer % 2, :, pl.ds(0, width)],
            dst_ref=got.at[source, :, pl.ds(0, width)],
            send_sem=send_sem.at[0],
            recv_sem=row_sem.at[source],
            device_id={"lat": target},
            device_id_type=MESH,
        )

    near = jnp.minimum(lat, LATS - 1 - lat)

    def each_row_copy(action):
        for lo, hi, width_out, width_in in KINDS:

            @pl.when(jnp.logical_and(near >= lo, near < hi))
            def _(width_out=width_out, width_in=width_in):
                def one(target):
                    to_inner = is_inner(target)

                    @pl.when(jnp.logical_not(to_inner))
                    def _():
                        action(row_copy(lat, target, width_out, False))

                    if width_in:

                        @pl.when(to_inner)
                        def _():
                            action(row_copy(lat, target, width_in, True))

                def both(step, carry):
                    one(wrapped(lat + (32 - step), LATS))
                    one(wrapped(lat + (32 + step), LATS))
                    return carry

                one(wrapped(lat + 32, LATS))
                lax.fori_loop(1, 32, both, 0)

    each_row_copy(lambda copy: copy.start())

    base = jnp.where(inner, 168, 0) + own
    stride = jnp.where(inner, INNER, OUTER)
    slot = jnp.minimum(
        lax.broadcasted_iota(jnp.int32, (8, 128), 0), jnp.where(inner, 7, 3)
    )
    order = (base + stride * slot).astype(F32)
    cosines = []
    state = []
    for block in range(4):
        cosine_lat, sine_lat = legendre(order, 128 * block)
        cosines.append(cosine_lat)
        first = start_value(order, sine_lat)
        values[block, 0:8, :] = first
        state.append(first)
        state.append(jnp.zeros_like(first))

    def advance(trip, carry):
        carry = list(carry)
        for step in range(1, 9):
            offset = trip * 8 + step
            top, mixed = step_factors(order, order + offset.astype(F32))
            row = pl.multiple_of(offset * 8, 8)
            for block in range(4):
                current, previous = carry[2 * block], carry[2 * block + 1]
                following = top * cosines[block] * current - mixed * previous
                values[block, pl.ds(row, 8), :] = following
                carry[2 * block], carry[2 * block + 1] = following, current
        return tuple(carry)

    lax.fori_loop(0, 44, advance, tuple(state))
    weight = lat_weight(NLAT)

    def tabulate(depths):
        for slot in range(2 * len(depths)):
            depth = depths[slot // 2]
            wave = base + stride * slot
            factor = jnp.where(wave > 0, math.sqrt(2.0), 1.0).astype(F32)
            offset = lax.broadcasted_iota(jnp.int32, (depth, 128), 0)
            for block in range(4):
                lanes = slice(128 * block, 128 * (block + 1))
                table = values[block, pl.ds(slot, depth, stride=8), :]
                table = jnp.where(
                    offset + wave <= TRUNC, table * (weight[:, lanes] * factor), 0.0
                )
                basis[slot, 0:depth, lanes] = table.astype(BF16)

    def receive(to_inner):
        for lo, hi, width_out, width_in in KINDS:
            width = width_in if to_inner else width_out
            if width:

                def one(source, carry, width=width):
                    @pl.when(source != lat)
                    def _():
                        row_copy(source, lat, width, to_inner).wait_recv()

                    return carry

                lax.fori_loop(lo, hi, one, 0)
                lax.fori_loop(LATS - hi, LATS - lo, one, 0)

    def combine(depths, rows):
        first = 0
        for pair, depth in enumerate(depths):
            lo, hi = (16, 48) if pair >= 2 else (0, 64)
            data = got[lo:hi, :, pair * 128 : (pair + 1) * 128].astype(F32)
            data = data.reshape((hi - lo) * BLOCK, 128).astype(BF16)
            both = [
                lax.dot_general(
                    basis[2 * pair + side, 0:depth, lo * BLOCK : hi * BLOCK],
                    data,
                    (((1,), (0,)), ((), ())),
                    preferred_element_type=F32,
                )
                for side in range(2)
            ]
            lane = lax.broadcasted_iota(jnp.int32, (depth, 128), 1)
            coef[first : first + depth, :] = jnp.where(lane < 64, both[0], both[1]).astype(BF16)
            first += depth
        coef[first:rows, :] = jnp.zeros((rows - first, 128), BF16)

    def month_copy(source, target, part):
        return pltpu.make_async_remote_copy(
            src_ref=coef.at[pl.ds(pl.multiple_of(target * part, part), part), :],
            dst_ref=share.at[source, pl.ds(0, part), :],
            send_sem=send_sem.at[1],
            recv_sem=month_sem.at[source],
            device_id={"tm": target},
            device_id_type=MESH,
        )

    def months(part):
        steps = (4, 3, 5, 2, 6, 1, 7)
        for step in steps:
            month_copy(tm, wrapped(tm + step, TMS), part).start()
        share[tm, 0:part, :] = coef[pl.ds(pl.multiple_of(tm * part, part), part), :]
        for step in steps[::-1]:
            month_copy(wrapped(tm + step, TMS), tm, part).wait_recv()
        pieces = [share[source, 0:part, :].astype(F32) for source in range(TMS)]
        columns = regroup(pieces).astype(BF16)
        terms = lax.dot_general(
            columns, columns, (((0,), (0,)), ((), ())), preferred_element_type=F32
        )
        row = lax.broadcasted_iota(jnp.int32, (MONTHS, MONTHS), 0)
        col = lax.broadcasted_iota(jnp.int32, (MONTHS, MONTHS), 1)
        diagonal = jnp.where(row == col, terms, 0.0)
        trace = jnp.sum(jnp.sum(diagonal, axis=0, keepdims=True), axis=1, keepdims=True)
        spare = jnp.logical_and((row & 3) == 1, col == row - 1)
        terms = jnp.where(spare, trace, terms)
        for odd, value in enumerate(exchange_halves(terms[:, :128], terms[:, 128:])):
            gram[:, odd] = value.reshape(32, 8, 128)

    @pl.when(outer)
    def _():
        tabulate(DEPTH_OUT)
        receive(False)
        combine(DEPTH_OUT, TMS * PART_OUT)
        months(PART_OUT)

    @pl.when(inner)
    def _():
        tabulate(DEPTH_IN)
        receive(True)
        combine(DEPTH_IN, TMS * PART_IN)
        months(PART_IN)

    me = tm * 8 + x * 2 + half
    y = tm // 2
    core = tm % 2
    plane = (z - half) * NX

    def slab_copy(source, target_y, target_core, target_x, target_half):
        target = target_y * 2 + target_core
        return pltpu.make_async_remote_copy(
            src_ref=gram.at[target * NX + target_x, target_half],
            dst_ref=slabs.at[source],
            send_sem=send_sem.at[2],
            recv_sem=slab_sem.at[source],
            device_id={"lat": plane + target_half * NX + target_x, "tm": target},
            device_id_type=MESH,
        )

    def others(away_first, action):
        order = (2, 1, 3, 0)
        for away_y in order if away_first else order[::-1]:
            peer_y = wrapped(y + away_y, 4)
            for away_x in order if away_first else order[::-1]:
                peer_x = wrapped(x + away_x, 4)
                for peer_half in (1 - half, half) if away_first else (half, 1 - half):
                    for peer_core in (1 - core, core):
                        here = away_y == 0 and away_x == 0
                        if not (here and peer_half is half and peer_core is core):
                            action(peer_y, peer_core, peer_x, peer_half)

    others(True, lambda *peer: slab_copy(me, *peer).start())
    slabs[me] = gram[me // 2, me % 2]

    def receive_slab(peer_y, peer_core, peer_x, peer_half):
        source = (peer_y * 2 + peer_core) * 8 + peer_x * 2 + peer_half
        slab_copy(source, y, core, x, half).wait_recv()

    others(False, receive_slab)
    own_pair = z // 2
    planes[own_pair] = jnp.sum(slabs[...], axis=0)

    def plane_copy(source, target):
        return pltpu.make_async_remote_copy(
            src_ref=planes.at[own_pair],
            dst_ref=planes.at[source],
            send_sem=send_sem.at[3],
            recv_sem=plane_sem.at[source],
            device_id={"lat": (target * 2 + half) * NX + x},
            device_id_type=MESH,
        )

    for away in (4, 3, 5, 2, 6, 1, 7):
        plane_copy(own_pair, wrapped(own_pair + away, 8)).start()

    each_row_copy(lambda copy: copy.wait_send())
    for applies, part in ((outer, PART_OUT), (inner, PART_IN)):

        @pl.when(applies)
        def _(part=part):
            for step in range(1, TMS):
                month_copy(tm, wrapped(tm + step, TMS), part).wait_send()

    def slab_sent(step, carry):
        slab_copy(me, y, core, x, half).wait_send()
        return carry

    lax.fori_loop(1, 64, slab_sent, 0)

    for away in range(1, 8):
        plane_copy(wrapped(own_pair + away, 8), own_pair).wait_recv()
    slab = jnp.sum(planes[...], axis=0)
    later = me // 32
    row = lax.broadcasted_iota(jnp.int32, (8, 128), 0) - 4 * later
    col = lax.broadcasted_iota(jnp.int32, (8, 128), 1) - (4 * me - 128 * later)
    spare = jnp.logical_and(row == 1, col == 0)
    twin = jnp.logical_and(row == 0, col == 1)

    def pick(mask):
        chosen = jnp.sum(jnp.where(mask, slab, 0.0), axis=0, keepdims=True)
        return jnp.sum(chosen, axis=1, keepdims=True)

    total = pick(spare)
    place = x * 2 + half
    finals[place] = jnp.where(spare, pick(twin), slab) * (MONTHS / (total + 1e-06))

    def last_copy(source, target):
        return pltpu.make_async_remote_copy(
            src_ref=finals.at[place],
            dst_ref=finals.at[source],
            send_sem=send_sem.at[4],
            recv_sem=last_sem.at[source],
            device_id={"lat": (z - half + target % 2) * NX + target // 2},
            device_id_type=MESH,
        )

    for away in (4, 5, 3, 2, 6, 1, 7):
        last_copy(place, wrapped(place + away, 8)).start()
    for away in range(1, 8):
        plane_copy(own_pair, wrapped(own_pair + away, 8)).wait_send()
    for away in range(1, 8):
        last_copy(wrapped(place + away, 8), place).wait_recv()
    for index in range(4):
        left, right = exchange_halves(finals[2 * index], finals[2 * index + 1])
        out_ref[8 * index : 8 * (index + 1), 0:128] = left
        out_ref[8 * index : 8 * (index + 1), 128:256] = right
    for away in range(1, 8):
        last_copy(place, wrapped(place + away, 8)).wait_send()


def local(fields):
    return pl.pallas_call(
        kernel,
        out_shape=jax.ShapeDtypeStruct((LOCAL, MONTHS), F32),
        in_specs=[pl.BlockSpec(memory_space=pltpu.HBM)],
        out_specs=pl.BlockSpec(memory_space=pltpu.VMEM),
        scratch_shapes=[
            pltpu.VMEM((BLOCK, LOCAL, NLON), BF16),
            pltpu.VMEM((12, 8, NLON), F32),
            pltpu.VMEM((736, NLON), BF16),
            pltpu.VMEM((PITCH_OUT // 2, 2, BLOCK, 256), BF16),
            pltpu.VMEM((PITCH_IN // 2, 2, BLOCK, 512), BF16),
            pltpu.VMEM((LATS, BLOCK, 512), BF16),
            pltpu.VMEM((4, 353 * 8, 128), F32),
            pltpu.VMEM((8, 352, NLAT), BF16),
            pltpu.VMEM((TMS * PART_OUT, 128), BF16),
            pltpu.VMEM((TMS, PART_OUT, 128), BF16),
            pltpu.VMEM((32, 2, 8, 128), F32),
            pltpu.VMEM((64, 8, 128), F32),
            pltpu.VMEM((8, 8, 128), F32),
            pltpu.VMEM((8, 8, 128), F32),
            pltpu.SemaphoreType.DMA,
            pltpu.SemaphoreType.DMA((5,)),
            pltpu.SemaphoreType.DMA((LATS,)),
            pltpu.SemaphoreType.DMA((TMS,)),
            pltpu.SemaphoreType.DMA((64,)),
            pltpu.SemaphoreType.DMA((8,)),
            pltpu.SemaphoreType.DMA((8,)),
        ],
        compiler_params=pltpu.CompilerParams(
            collective_id=0, has_side_effects=True, vmem_limit_bytes=67_043_328
        ),
    )(fields)


def solution(mesh):
    return jax.shard_map(
        local,
        mesh=mesh,
        in_specs=(P("lat", "tm", None),),
        out_specs=P("tm", None),
        check_vma=False,
    )
```

```python
import functools
import math

import jax
import jax.numpy as jnp
from jax import lax
from jax.experimental import pallas as pl
from jax.experimental.pallas import tpu as pltpu
from jax.sharding import PartitionSpec as P

TRUNC = 341
NLON = 1024
NLAT = 512
MONTHS = 256
LATS = 64
TMS = 8
NX = 4
BLOCK = 8
LOCAL = 32
MIDDLE = 19
INNER = 22
OUTER = 42
DEPTH_OUT = (352, 272)
DEPTH_IN = (176, 144, 96, 48)
PART_OUT = 80
PART_IN = 64
PITCH_OUT = 44
PITCH_IN = 24
KINDS = (
    (0, 9, 128, 0),
    (9, 14, 256, 0),
    (14, 16, 256, 128),
    (16, 17, 256, 256),
    (17, 18, 256, 384),
    (18, 32, 256, 512),
)
MESH = pl.DeviceIdType.MESH
F32 = jnp.float32
BF16 = jnp.bfloat16
SINE = tuple(
    (-1.0) ** k * (2.0 * math.pi) ** (2 * k + 1) / math.factorial(2 * k + 1) for k in range(7)
)


def sine_of_turns(u):
    square = u * u
    total = jnp.full_like(u, SINE[6])
    for k in range(5, -1, -1):
        total = total * square + SINE[k]
    return total * u


def cosine_of_phase(phase):
    away = jnp.abs(((phase + 512) & 1023) - 512)
    return sine_of_turns((256 - away).astype(F32) * (1.0 / NLON))


def waves_times_lon(first, slot_step, owner_step, part_step):
    sub = lax.broadcasted_iota(jnp.int32, (8, NLON), 0)
    lon = lax.broadcasted_iota(jnp.int32, (8, NLON), 1)
    wave = first + slot_step * ((sub >> 1) & 1) + owner_step * (sub >> 2)
    return wave * lon + part_step * (sub & 1)


def cosine_sine(phase):
    return cosine_of_phase(phase), cosine_of_phase(phase - 256)


def turn(pair, by):
    cosine, sine = pair
    return cosine * by[0] - sine * by[1], sine * by[0] + cosine * by[1]


def roll(value, shift, axis):
    return pltpu.roll(value, shift % value.shape[axis], axis)


def swap_bit(value, bit):
    rows = value.shape[0]
    sub = (lax.broadcasted_iota(jnp.int32, (rows, 128), 0) >> bit) & 1
    group = (lax.broadcasted_iota(jnp.int32, (rows, 128), 1) >> (5 + bit)) & 1
    step = 1 << bit
    from_below = roll(roll(value, 32 * step, 1), -step, 0)
    from_above = roll(roll(value, -32 * step, 1), step, 0)
    return jnp.where(sub == group, value, jnp.where(sub == 0, from_below, from_above))


def rows_by_latitude(spectrum):
    low, high = spectrum[:, :128], spectrum[:, 128:]
    return [swap_bit(swap_bit(part, 0), 1) for part in exchange_halves(low, high)]


def start_value(order, sine_lat):
    ratio = jnp.ones_like(order)
    for step in range(1, 9):
        ratio = ratio * ((order + step) / (order + (step + 0.5)))
    far = order + 9.0
    inverse = 1.0 / far
    square = inverse * inverse
    series = inverse * (-1.0 / 8.0 + square * (1.0 / 192.0 - square * (1.0 / 640.0)))
    log_ratio = 0.5 * jnp.log(far) + series + jnp.log(ratio)
    constant = math.log(0.5) - (0.5 * math.log(math.pi) - math.log(2.0))
    log_start = 0.5 * (constant + log_ratio) + order * jnp.log(sine_lat)
    taper = jnp.clip((log_start + 70.0) / 10.0, 0.0, 1.0)
    return jnp.exp(jnp.maximum(log_start, -80.0)) * taper


def step_factors(order, degree):
    top = jnp.sqrt((4.0 * degree * degree - 1.0) / (degree * degree - order * order))
    below = degree - 1.0
    back = jnp.sqrt(
        jnp.maximum(below * below - order * order, 0.0) / jnp.abs(4.0 * below * below - 1.0)
    )
    return top, top * back


def legendre(waves, lane_offset):
    place = (lax.broadcasted_iota(jnp.int32, (8, 128), 1) + lane_offset).astype(F32) + 0.5
    turns = place * (0.5 / NLAT)
    folded = jnp.minimum(turns, 0.5 - turns)
    half = sine_of_turns(0.5 * folded)
    cosine = jnp.where(folded < 0.125, 1.0 - 2.0 * half * half, sine_of_turns(0.25 - folded))
    return jnp.where(turns < 0.25, cosine, -cosine), sine_of_turns(folded)


def lat_weight(width):
    turns = (lax.broadcasted_iota(jnp.int32, (1, width), 1).astype(F32) + 0.5) * (0.5 / NLAT)
    return sine_of_turns(jnp.minimum(turns, 0.5 - turns)) * (math.pi / NLAT)


def regroup(pieces):
    group = lax.broadcasted_iota(jnp.int32, pieces[0].shape, 1) >> 5
    blocks = []
    for g in range(4):
        halves = []
        for half in range(2):
            total = None
            for a in range(4):
                moved = pieces[4 * half + a]
                if a != g:
                    moved = roll(moved, 32 * (a - g), 1)
                total = moved if total is None else jnp.where(group == a, moved, total)
            halves.append(total)
        blocks.append(jnp.concatenate(halves, axis=1))
    return jnp.concatenate(blocks, axis=0)


def exchange_halves(left, right):
    upper = ((lax.broadcasted_iota(jnp.int32, left.shape, 0) >> 2) & 1) == 0
    return (
        jnp.where(upper, left, roll(right, 4, 0)),
        jnp.where(upper, roll(left, -4, 0), right),
    )


def wrapped(value, length):
    return jnp.where(value >= length, value - length, value)


def is_inner(lat):
    return jnp.logical_and(lat >= MIDDLE, lat < MIDDLE + INNER)


def outer_owner(lat):
    return jnp.where(lat < MIDDLE, lat, lat - INNER)


def kernel(
    fields_hbm,
    out_ref,
    fields,
    patterns,
    transform,
    send_out,
    send_in,
    got,
    values,
    basis,
    coef,
    share,
    gram,
    slabs,
    planes,
    finals,
    local_sem,
    send_sem,
    row_sem,
    month_sem,
    slab_sem,
    plane_sem,
    last_sem,
):
    lat = lax.axis_index("lat")
    tm = lax.axis_index("tm")
    z = lat // NX
    x = lat % NX
    half = z % 2
    inner = is_inner(lat)
    outer = jnp.logical_not(inner)
    load = pltpu.make_async_copy(fields_hbm, fields, local_sem)
    load.start()
    got[...] = jnp.zeros_like(got)

    barrier = pltpu.get_barrier_semaphore()
    for away in range(32, 0, -1):
        for step in {away, LATS - away}:
            pl.semaphore_signal(
                barrier,
                inc=1,
                device_id={"lat": wrapped(lat + step, LATS)},
                device_id_type=MESH,
            )
    for step in range(1, TMS):
        pl.semaphore_signal(
            barrier, inc=1, device_id={"tm": wrapped(tm + step, TMS)}, device_id_type=MESH
        )

    for index in range(6):
        if index < 2:
            phase = waves_times_lon(2 * OUTER * index, OUTER, 0, 256)
        else:
            phase = waves_times_lon(168 + 2 * INNER * (index - 2), INNER, 0, 256)
        cosine, sine = cosine_sine(phase)
        patterns[2 * index] = cosine * (1.0 / math.sqrt(NLON))
        patterns[2 * index + 1] = sine * (1.0 / math.sqrt(NLON))
    by = cosine_sine(waves_times_lon(2, 0, 0, 0))

    def fill(kinds, trip, pair):
        following = turn(pair, by)
        for index in kinds:
            first = 176 * index if index < 2 else 352 + 96 * (index - 2)
            rows = [
                cosine * patterns[2 * index] - sine * patterns[2 * index + 1]
                for cosine, sine in (pair, following)
            ]
            start = pl.multiple_of(first + trip * 16, 16)
            transform[pl.ds(start, 16), :] = jnp.concatenate(rows, axis=0).astype(BF16)
        return turn(following, by)

    pair = cosine_sine(waves_times_lon(0, 0, 1, 0))
    pair = lax.fori_loop(0, 6, functools.partial(fill, range(6)), pair)
    lax.fori_loop(6, 11, functools.partial(fill, range(2)), pair)
    load.wait()
    flat = fields[...].reshape(BLOCK * LOCAL, NLON)
    for index in range(6):
        first, rows, buffer, place = (
            (176 * index, 176, send_out, index)
            if index < 2
            else (352 + 96 * (index - 2), 96, send_in, index - 2)
        )
        spectrum = lax.dot_general(
            transform[first : first + rows, :],
            flat,
            (((1,), (1,)), ((), ())),
            preferred_element_type=F32,
        )
        for odd, part in enumerate(rows_by_latitude(spectrum)):
            buffer[:, odd, :, place * 128 : (place + 1) * 128] = part.reshape(
                rows // 8, BLOCK, 128
            ).astype(BF16)

    own = jnp.where(inner, lat - MIDDLE, outer_owner(lat))

    @pl.when(inner)
    def _():
        got[lat] = send_in[own // 2, own % 2]

    @pl.when(outer)
    def _():
        got[lat, :, 0:256] = send_out[own // 2, own % 2]

    pl.semaphore_wait(barrier, LATS - 1 + TMS - 1)

    def row_copy(source, target, width, to_inner):
        if to_inner:
            peer = target - MIDDLE
            buffer = send_in
        else:
            peer = outer_owner(target)
            buffer = send_out
        return pltpu.make_async_remote_copy(
            src_ref=buffer.at[peer // 2, peer % 2, :, pl.ds(0, width)],
            dst_ref=got.at[source, :, pl.ds(0, width)],
            send_sem=send_sem.at[0],
            recv_sem=row_sem.at[source],
            device_id={"lat": target},
            device_id_type=MESH,
        )

    near = jnp.minimum(lat, LATS - 1 - lat)

    def each_row_copy(action):
        for lo, hi, width_out, width_in in KINDS:

            @pl.when(jnp.logical_and(near >= lo, near < hi))
            def _(width_out=width_out, width_in=width_in):
                def one(target):
                    to_inner = is_inner(target)

                    @pl.when(jnp.logical_not(to_inner))
                    def _():
                        action(row_copy(lat, target, width_out, False))

                    if width_in:

                        @pl.when(to_inner)
                        def _():
                            action(row_copy(lat, target, width_in, True))

                def both(step, carry):
                    one(wrapped(lat + (32 - step), LATS))
                    one(wrapped(lat + (32 + step), LATS))
                    return carry

                one(wrapped(lat + 32, LATS))
                lax.fori_loop(1, 32, both, 0)

    each_row_copy(lambda copy: copy.start())

    base = jnp.where(inner, 168, 0) + own
    stride = jnp.where(inner, INNER, OUTER)
    slot = jnp.minimum(
        lax.broadcasted_iota(jnp.int32, (8, 128), 0), jnp.where(inner, 7, 3)
    )
    order = (base + stride * slot).astype(F32)
    cosines = []
    state = []
    for block in range(4):
        cosine_lat, sine_lat = legendre(order, 128 * block)
        cosines.append(cosine_lat)
        first = start_value(order, sine_lat)
        values[block, 0:8, :] = first
        state.append(first)
        state.append(jnp.zeros_like(first))

    def advance(trip, carry):
        carry = list(carry)
        for step in range(1, 9):
            offset = trip * 8 + step
            top, mixed = step_factors(order, order + offset.astype(F32))
            row = pl.multiple_of(offset * 8, 8)
            for block in range(4):
                current, previous = carry[2 * block], carry[2 * block + 1]
                following = top * cosines[block] * current - mixed * previous
                values[block, pl.ds(row, 8), :] = following
                carry[2 * block], carry[2 * block + 1] = following, current
        return tuple(carry)

    lax.fori_loop(0, 44, advance, tuple(state))
    weight = lat_weight(NLAT)

    def tabulate(depths):
        for slot in range(2 * len(depths)):
            depth = depths[slot // 2]
            wave = base + stride * slot
            factor = jnp.where(wave > 0, math.sqrt(2.0), 1.0).astype(F32)
            offset = lax.broadcasted_iota(jnp.int32, (depth, 128), 0)
            for block in range(4):
                lanes = slice(128 * block, 128 * (block + 1))
                table = values[block, pl.ds(slot, depth, stride=8), :]
                table = jnp.where(
                    offset + wave <= TRUNC, table * (weight[:, lanes] * factor), 0.0
                )
                basis[slot, 0:depth, lanes] = table.astype(BF16)

    def receive(to_inner):
        for lo, hi, width_out, width_in in KINDS:
            width = width_in if to_inner else width_out
            if width:

                def one(source, carry, width=width):
                    @pl.when(source != lat)
                    def _():
                        row_copy(source, lat, width, to_inner).wait_recv()

                    return carry

                lax.fori_loop(lo, hi, one, 0)
                lax.fori_loop(LATS - hi, LATS - lo, one, 0)

    def combine(depths, rows):
        first = 0
        for pair, depth in enumerate(depths):
            lo, hi = (16, 48) if pair >= 2 else (0, 64)
            data = got[lo:hi, :, pair * 128 : (pair + 1) * 128]
            data = data.reshape((hi - lo) * BLOCK, 128)
            both = [
                lax.dot_general(
                    basis[2 * pair + side, 0:depth, lo * BLOCK : hi * BLOCK],
                    data,
                    (((1,), (0,)), ((), ())),
                    preferred_element_type=F32,
                )
                for side in range(2)
            ]
            lane = lax.broadcasted_iota(jnp.int32, (depth, 128), 1)
            coef[first : first + depth, :] = jnp.where(lane < 64, both[0], both[1]).astype(BF16)
            first += depth
        coef[first:rows, :] = jnp.zeros((rows - first, 128), BF16)

    def month_copy(source, target, part):
        return pltpu.make_async_remote_copy(
            src_ref=coef.at[pl.ds(pl.multiple_of(target * part, part), part), :],
            dst_ref=share.at[source, pl.ds(0, part), :],
            send_sem=send_sem.at[1],
            recv_sem=month_sem.at[source],
            device_id={"tm": target},
            device_id_type=MESH,
        )

    def months(part):
        steps = (4, 3, 5, 2, 6, 1, 7)
        for step in steps:
            month_copy(tm, wrapped(tm + step, TMS), part).start()
        share[tm, 0:part, :] = coef[pl.ds(pl.multiple_of(tm * part, part), part), :]
        for step in steps[::-1]:
            month_copy(wrapped(tm + step, TMS), tm, part).wait_recv()
        pieces = [share[source, 0:part, :].astype(F32) for source in range(TMS)]
        columns = regroup(pieces).astype(BF16)
        terms = lax.dot_general(
            columns, columns, (((0,), (0,)), ((), ())), preferred_element_type=F32
        )
        row = lax.broadcasted_iota(jnp.int32, (MONTHS, MONTHS), 0)
        col = lax.broadcasted_iota(jnp.int32, (MONTHS, MONTHS), 1)
        squares = functools.reduce(jnp.add, [piece * piece for piece in pieces])
        trace = jnp.sum(jnp.sum(squares, axis=0, keepdims=True), axis=1, keepdims=True)
        spare = jnp.logical_and((row & 3) == 1, col == row - 1)
        terms = jnp.where(spare, trace, terms)
        for odd, value in enumerate(exchange_halves(terms[:, :128], terms[:, 128:])):
            gram[:, odd] = value.reshape(32, 8, 128)

    @pl.when(outer)
    def _():
        tabulate(DEPTH_OUT)
        receive(False)
        combine(DEPTH_OUT, TMS * PART_OUT)
        months(PART_OUT)

    @pl.when(inner)
    def _():
        tabulate(DEPTH_IN)
        receive(True)
        combine(DEPTH_IN, TMS * PART_IN)
        months(PART_IN)

    me = tm * 8 + x * 2 + half
    y = tm // 2
    core = tm % 2
    plane = (z - half) * NX

    def slab_copy(source, target_y, target_core, target_x, target_half):
        target = target_y * 2 + target_core
        return pltpu.make_async_remote_copy(
            src_ref=gram.at[target * NX + target_x, target_half],
            dst_ref=slabs.at[source],
            send_sem=send_sem.at[2],
            recv_sem=slab_sem.at[source],
            device_id={"lat": plane + target_half * NX + target_x, "tm": target},
            device_id_type=MESH,
        )

    def others(away_first, action):
        order = (2, 1, 3, 0)
        for away_y in order if away_first else order[::-1]:
            peer_y = wrapped(y + away_y, 4)
            for away_x in order if away_first else order[::-1]:
                peer_x = wrapped(x + away_x, 4)
                for peer_half in (1 - half, half) if away_first else (half, 1 - half):
                    for peer_core in (1 - core, core):
                        here = away_y == 0 and away_x == 0
                        if not (here and peer_half is half and peer_core is core):
                            action(peer_y, peer_core, peer_x, peer_half)

    others(True, lambda *peer: slab_copy(me, *peer).start())
    slabs[me] = gram[me // 2, me % 2]

    def receive_slab(peer_y, peer_core, peer_x, peer_half):
        source = (peer_y * 2 + peer_core) * 8 + peer_x * 2 + peer_half
        slab_copy(source, y, core, x, half).wait_recv()

    others(False, receive_slab)
    own_pair = z // 2
    planes[own_pair] = jnp.sum(slabs[...], axis=0)

    def plane_copy(source, target):
        return pltpu.make_async_remote_copy(
            src_ref=planes.at[own_pair],
            dst_ref=planes.at[source],
            send_sem=send_sem.at[3],
            recv_sem=plane_sem.at[source],
            device_id={"lat": (target * 2 + half) * NX + x},
            device_id_type=MESH,
        )

    for away in (4, 3, 5, 2, 6, 1, 7):
        plane_copy(own_pair, wrapped(own_pair + away, 8)).start()

    each_row_copy(lambda copy: copy.wait_send())
    for applies, part in ((outer, PART_OUT), (inner, PART_IN)):

        @pl.when(applies)
        def _(part=part):
            for step in range(1, TMS):
                month_copy(tm, wrapped(tm + step, TMS), part).wait_send()

    def slab_sent(step, carry):
        slab_copy(me, y, core, x, half).wait_send()
        return carry

    lax.fori_loop(1, 64, slab_sent, 0)

    for away in range(1, 8):
        plane_copy(wrapped(own_pair + away, 8), own_pair).wait_recv()
    slab = jnp.sum(planes[...], axis=0)
    later = me // 32
    row = lax.broadcasted_iota(jnp.int32, (8, 128), 0) - 4 * later
    col = lax.broadcasted_iota(jnp.int32, (8, 128), 1) - (4 * me - 128 * later)
    spare = jnp.logical_and(row == 1, col == 0)

    place = x * 2 + half
    finals[place] = jnp.where(spare, roll(roll(slab, 1, 0), -1, 1), slab)

    def last_copy(source, target):
        return pltpu.make_async_remote_copy(
            src_ref=finals.at[place],
            dst_ref=finals.at[source],
            send_sem=send_sem.at[4],
            recv_sem=last_sem.at[source],
            device_id={"lat": (z - half + target % 2) * NX + target // 2},
            device_id_type=MESH,
        )

    for away in (4, 5, 3, 2, 6, 1, 7):
        last_copy(place, wrapped(place + away, 8)).start()
    for away in range(1, 8):
        plane_copy(own_pair, wrapped(own_pair + away, 8)).wait_send()
    chosen = jnp.sum(jnp.where(spare, slab, 0.0), axis=0, keepdims=True)
    scale = MONTHS / (jnp.sum(chosen, axis=1, keepdims=True) + 1e-06)
    for away in range(1, 8):
        last_copy(wrapped(place + away, 8), place).wait_recv()
    for index in range(4):
        left, right = exchange_halves(finals[2 * index], finals[2 * index + 1])
        out_ref[8 * index : 8 * (index + 1), 0:128] = left * scale
        out_ref[8 * index : 8 * (index + 1), 128:256] = right * scale
    for away in range(1, 8):
        last_copy(place, wrapped(place + away, 8)).wait_send()


def local(fields):
    return pl.pallas_call(
        kernel,
        out_shape=jax.ShapeDtypeStruct((LOCAL, MONTHS), F32),
        in_specs=[pl.BlockSpec(memory_space=pltpu.HBM)],
        out_specs=pl.BlockSpec(memory_space=pltpu.VMEM),
        scratch_shapes=[
            pltpu.VMEM((BLOCK, LOCAL, NLON), BF16),
            pltpu.VMEM((12, 8, NLON), F32),
            pltpu.VMEM((736, NLON), BF16),
            pltpu.VMEM((PITCH_OUT // 2, 2, BLOCK, 256), BF16),
            pltpu.VMEM((PITCH_IN // 2, 2, BLOCK, 512), BF16),
            pltpu.VMEM((LATS, BLOCK, 512), BF16),
            pltpu.VMEM((4, 353 * 8, 128), F32),
            pltpu.VMEM((8, 352, NLAT), BF16),
            pltpu.VMEM((TMS * PART_OUT, 128), BF16),
            pltpu.VMEM((TMS, PART_OUT, 128), BF16),
            pltpu.VMEM((32, 2, 8, 128), F32),
            pltpu.VMEM((64, 8, 128), F32),
            pltpu.VMEM((8, 8, 128), F32),
            pltpu.VMEM((8, 8, 128), F32),
            pltpu.SemaphoreType.DMA,
            pltpu.SemaphoreType.DMA((5,)),
            pltpu.SemaphoreType.DMA((LATS,)),
            pltpu.SemaphoreType.DMA((TMS,)),
            pltpu.SemaphoreType.DMA((64,)),
            pltpu.SemaphoreType.DMA((8,)),
            pltpu.SemaphoreType.DMA((8,)),
        ],
        compiler_params=pltpu.CompilerParams(
            collective_id=0, has_side_effects=True, vmem_limit_bytes=67_043_328
        ),
    )(fields)


def solution(mesh):
    return jax.shard_map(
        local,
        mesh=mesh,
        in_specs=(P("lat", "tm", None),),
        out_specs=P("tm", None),
        check_vma=False,
    )
```

```python
import functools
import math

import jax
import jax.numpy as jnp
from jax import lax
from jax.experimental import pallas as pl
from jax.experimental.pallas import tpu as pltpu
from jax.sharding import PartitionSpec as P

TRUNC = 341
NLON = 1024
NLAT = 512
MONTHS = 256
LATS = 64
TMS = 8
NX = 4
BLOCK = 8
LOCAL = 32
MIDDLE = 23
INNER = 16
IDLE = 2
OUTER = 46
FIRST_IN = 4 * OUTER
DEPTH_OUT = (352, 256)
DEPTH_IN = (160, 128, 96, 64, 32)
PART_OUT = 80
PART_IN = 64
PITCH_OUT = 48
PITCH_IN = 16
PAIRS_OUT = len(DEPTH_OUT)
PAIRS = PAIRS_OUT + len(DEPTH_IN)
LANES_IN = 128 * len(DEPTH_IN)
KINDS = (
    (0, 9, 128, 0),
    (9, 15, 256, 0),
    (15, 16, 256, 128),
    (16, 17, 256, 256),
    (17, 18, 256, 384),
    (18, 32, 256, 640),
)
MESH = pl.DeviceIdType.MESH
F32 = jnp.float32
BF16 = jnp.bfloat16
SINE = tuple(
    (-1.0) ** k * (2.0 * math.pi) ** (2 * k + 1) / math.factorial(2 * k + 1) for k in range(7)
)


def sine_of_turns(u):
    square = u * u
    total = jnp.full_like(u, SINE[6])
    for k in range(5, -1, -1):
        total = total * square + SINE[k]
    return total * u


def cosine_of_phase(phase):
    away = jnp.abs(((phase + 512) & 1023) - 512)
    return sine_of_turns((256 - away).astype(F32) * (1.0 / NLON))


def waves_times_lon(first, slot_step, owner_step, part_step):
    sub = lax.broadcasted_iota(jnp.int32, (8, NLON), 0)
    lon = lax.broadcasted_iota(jnp.int32, (8, NLON), 1)
    wave = first + slot_step * ((sub >> 1) & 1) + owner_step * (sub >> 2)
    return wave * lon + part_step * (sub & 1)


def cosine_sine(phase):
    return cosine_of_phase(phase), cosine_of_phase(phase - 256)


def turn(pair, by):
    cosine, sine = pair
    return cosine * by[0] - sine * by[1], sine * by[0] + cosine * by[1]


def roll(value, shift, axis):
    return pltpu.roll(value, shift % value.shape[axis], axis)


def swap_bit(value, bit):
    rows = value.shape[0]
    sub = (lax.broadcasted_iota(jnp.int32, (rows, 128), 0) >> bit) & 1
    group = (lax.broadcasted_iota(jnp.int32, (rows, 128), 1) >> (5 + bit)) & 1
    step = 1 << bit
    down = roll(value, 32 * step, 1)
    up = down if step == 2 else roll(value, -32 * step, 1)
    from_below = roll(down, -step, 0)
    from_above = roll(up, step, 0)
    return jnp.where(sub == group, value, jnp.where(sub == 0, from_below, from_above))


def rows_by_latitude(spectrum):
    low, high = spectrum[:, :128], spectrum[:, 128:]
    return [swap_bit(swap_bit(part, 0), 1) for part in exchange_halves(low, high)]


def start_value(order, sine_lat):
    ratio = jnp.ones_like(order)
    for step in range(1, 9):
        ratio = ratio * ((order + step) / (order + (step + 0.5)))
    far = order + 9.0
    inverse = 1.0 / far
    square = inverse * inverse
    series = inverse * (-1.0 / 8.0 + square * (1.0 / 192.0 - square * (1.0 / 640.0)))
    log_ratio = 0.5 * jnp.log(far) + series + jnp.log(ratio)
    constant = math.log(0.5) - (0.5 * math.log(math.pi) - math.log(2.0))
    log_start = 0.5 * (constant + log_ratio) + order * jnp.log(sine_lat)
    taper = jnp.clip((log_start + 70.0) / 10.0, 0.0, 1.0)
    return jnp.exp(jnp.maximum(log_start, -80.0)) * taper


def step_factors(order, degree):
    top = jnp.sqrt((4.0 * degree * degree - 1.0) / (degree * degree - order * order))
    below = degree - 1.0
    back = jnp.sqrt(
        jnp.maximum(below * below - order * order, 0.0) / jnp.abs(4.0 * below * below - 1.0)
    )
    return top, top * back


def legendre(waves, lane_offset):
    place = (lax.broadcasted_iota(jnp.int32, (8, 128), 1) + lane_offset).astype(F32) + 0.5
    turns = place * (0.5 / NLAT)
    folded = jnp.minimum(turns, 0.5 - turns)
    half = sine_of_turns(0.5 * folded)
    cosine = jnp.where(folded < 0.125, 1.0 - 2.0 * half * half, sine_of_turns(0.25 - folded))
    return jnp.where(turns < 0.25, cosine, -cosine), sine_of_turns(folded)


def lat_weight(width):
    turns = (lax.broadcasted_iota(jnp.int32, (1, width), 1).astype(F32) + 0.5) * (0.5 / NLAT)
    return sine_of_turns(jnp.minimum(turns, 0.5 - turns)) * (math.pi / NLAT)


def regroup(pieces):
    group = lax.broadcasted_iota(jnp.int32, pieces[0].shape, 1) >> 5
    blocks = []
    for g in range(4):
        halves = []
        for half in range(2):
            total = None
            for a in range(4):
                moved = pieces[4 * half + a]
                if a != g:
                    moved = roll(moved, 32 * (a - g), 1)
                total = moved if total is None else jnp.where(group == a, moved, total)
            halves.append(total)
        blocks.append(jnp.concatenate(halves, axis=1))
    return jnp.concatenate(blocks, axis=0)


def exchange_halves(left, right):
    upper = ((lax.broadcasted_iota(jnp.int32, left.shape, 0) >> 2) & 1) == 0
    return (
        jnp.where(upper, left, roll(right, 4, 0)),
        jnp.where(upper, roll(left, -4, 0), right),
    )


def wrapped(value, length):
    return jnp.where(value >= length, value - length, value)


def is_inner(lat):
    return jnp.logical_and(lat >= MIDDLE, lat < MIDDLE + INNER)


def is_outer(lat):
    return jnp.logical_or(lat < MIDDLE, lat >= MIDDLE + INNER + IDLE)


def outer_owner(lat):
    return jnp.where(lat < MIDDLE, lat, lat - INNER - IDLE)


def pair_rows(index):
    if index < PAIRS_OUT:
        return 4 * PITCH_OUT * index, 4 * PITCH_OUT
    return 4 * (PITCH_OUT * PAIRS_OUT + PITCH_IN * (index - PAIRS_OUT)), 4 * PITCH_IN


def kernel(
    fields_hbm,
    out_ref,
    fields,
    patterns,
    transform,
    send_out,
    send_in,
    got,
    values,
    more_values,
    basis,
    coef,
    share,
    gram,
    slabs,
    planes,
    finals,
    local_sem,
    send_sem,
    row_sem,
    month_sem,
    slab_sem,
    plane_sem,
    last_sem,
):
    lat = lax.axis_index("lat")
    tm = lax.axis_index("tm")
    z = lat // NX
    x = lat % NX
    half = z % 2
    inner = is_inner(lat)
    outer = is_outer(lat)
    load = pltpu.make_async_copy(fields_hbm, fields, local_sem)
    load.start()
    got[...] = jnp.zeros_like(got)

    barrier = pltpu.get_barrier_semaphore()
    for away in range(32, 0, -1):
        for step in {away, LATS - away}:
            pl.semaphore_signal(
                barrier,
                inc=1,
                device_id={"lat": wrapped(lat + step, LATS)},
                device_id_type=MESH,
            )
    for step in range(1, TMS):
        pl.semaphore_signal(
            barrier, inc=1, device_id={"tm": wrapped(tm + step, TMS)}, device_id_type=MESH
        )

    for index in range(PAIRS):
        if index < PAIRS_OUT:
            phase = waves_times_lon(2 * OUTER * index, OUTER, 0, 256)
        else:
            first = FIRST_IN + 2 * INNER * (index - PAIRS_OUT)
            phase = waves_times_lon(first, INNER, 0, 256)
        cosine, sine = cosine_sine(phase)
        patterns[2 * index] = cosine * (1.0 / math.sqrt(NLON))
        patterns[2 * index + 1] = sine * (1.0 / math.sqrt(NLON))
    by = cosine_sine(waves_times_lon(2, 0, 0, 0))

    def fill(kinds, trip, pair):
        following = turn(pair, by)
        for index in kinds:
            first, _ = pair_rows(index)
            rows = [
                cosine * patterns[2 * index] - sine * patterns[2 * index + 1]
                for cosine, sine in (pair, following)
            ]
            start = pl.multiple_of(first + trip * 16, 16)
            transform[pl.ds(start, 16), :] = jnp.concatenate(rows, axis=0).astype(BF16)
        return turn(following, by)

    pair = cosine_sine(waves_times_lon(0, 0, 1, 0))
    trips_in, trips_out = PITCH_IN // 4, PITCH_OUT // 4
    pair = lax.fori_loop(0, trips_in, functools.partial(fill, range(PAIRS)), pair)
    lax.fori_loop(trips_in, trips_out, functools.partial(fill, range(PAIRS_OUT)), pair)
    load.wait()
    flat = fields[...].reshape(BLOCK * LOCAL, NLON)
    for index in range(PAIRS):
        first, rows = pair_rows(index)
        if index < PAIRS_OUT:
            buffer, place = send_out, index
        else:
            buffer, place = send_in, index - PAIRS_OUT
        spectrum = lax.dot_general(
            transform[first : first + rows, :],
            flat,
            (((1,), (1,)), ((), ())),
            preferred_element_type=F32,
        )
        for odd, part in enumerate(rows_by_latitude(spectrum)):
            buffer[:, odd, :, place * 128 : (place + 1) * 128] = part.reshape(
                rows // 8, BLOCK, 128
            ).astype(BF16)

    own = jnp.where(inner, lat - MIDDLE, outer_owner(lat))

    @pl.when(inner)
    def _():
        got[lat] = send_in[own // 2, own % 2]

    @pl.when(outer)
    def _():
        got[lat, :, 0:256] = send_out[own // 2, own % 2]

    pl.semaphore_wait(barrier, LATS - 1 + TMS - 1)

    def row_copy(source, target, width, to_inner):
        if to_inner:
            peer = target - MIDDLE
            buffer = send_in
        else:
            peer = outer_owner(target)
            buffer = send_out
        return pltpu.make_async_remote_copy(
            src_ref=buffer.at[peer // 2, peer % 2, :, pl.ds(0, width)],
            dst_ref=got.at[source, :, pl.ds(0, width)],
            send_sem=send_sem.at[0],
            recv_sem=row_sem.at[source],
            device_id={"lat": target},
            device_id_type=MESH,
        )

    near = jnp.minimum(lat, LATS - 1 - lat)

    def each_row_copy(action):
        for lo, hi, width_out, width_in in KINDS:

            @pl.when(jnp.logical_and(near >= lo, near < hi))
            def _(width_out=width_out, width_in=width_in):
                def one(target):
                    to_inner = is_inner(target)

                    @pl.when(is_outer(target))
                    def _():
                        action(row_copy(lat, target, width_out, False))

                    if width_in:

                        @pl.when(to_inner)
                        def _():
                            action(row_copy(lat, target, width_in, True))

                def both(step, carry):
                    one(wrapped(lat + (32 - step), LATS))
                    one(wrapped(lat + (32 + step), LATS))
                    return carry

                one(wrapped(lat + 32, LATS))
                lax.fori_loop(1, 32, both, 0)

    each_row_copy(lambda copy: copy.start())

    base = jnp.where(inner, FIRST_IN + own, jnp.where(outer, own, 400))
    stride = jnp.where(inner, INNER, OUTER)
    slot = jnp.minimum(
        lax.broadcasted_iota(jnp.int32, (8, 128), 0), jnp.where(inner, 7, 3)
    )
    order = (base + stride * slot).astype(F32)
    def recur(order, table, trips):
        cosines = []
        state = []
        for block in range(4):
            cosine_lat, sine_lat = legendre(order, 128 * block)
            cosines.append(cosine_lat)
            first = start_value(order, sine_lat)
            table[block, 0:8, :] = first
            state.append(first)
            state.append(jnp.zeros_like(first))

        def advance(trip, carry):
            carry = list(carry)
            for step in range(1, 9):
                offset = trip * 8 + step
                top, mixed = step_factors(order, order + offset.astype(F32))
                row = pl.multiple_of(offset * 8, 8)
                for block in range(4):
                    current, previous = carry[2 * block], carry[2 * block + 1]
                    following = top * cosines[block] * current - mixed * previous
                    table[block, pl.ds(row, 8), :] = following
                    carry[2 * block], carry[2 * block + 1] = following, current
            return tuple(carry)

        lax.fori_loop(0, trips, advance, tuple(state))

    recur(order, values, 44)

    @pl.when(inner)
    def _():
        slot = 8 + jnp.minimum(lax.broadcasted_iota(jnp.int32, (8, 128), 0), 1)
        recur((base + stride * slot).astype(F32), more_values, 4)

    weight = lat_weight(NLAT)

    def tabulate(depths):
        for slot in range(2 * len(depths)):
            depth = depths[slot // 2]
            wave = base + stride * slot
            factor = jnp.where(wave > 0, math.sqrt(2.0), 1.0).astype(F32)
            offset = lax.broadcasted_iota(jnp.int32, (depth, 128), 0)
            for block in range(4):
                lanes = slice(128 * block, 128 * (block + 1))
                source = values if slot < 8 else more_values
                table = source[block, pl.ds(slot % 8, depth, stride=8), :]
                table = jnp.where(
                    offset + wave <= TRUNC, table * (weight[:, lanes] * factor), 0.0
                )
                basis[slot, 0:depth, lanes] = table.astype(BF16)

    def receive(to_inner):
        for lo, hi, width_out, width_in in KINDS:
            width = width_in if to_inner else width_out
            if width:

                def one(source, carry, width=width):
                    @pl.when(source != lat)
                    def _():
                        row_copy(source, lat, width, to_inner).wait_recv()

                    return carry

                lax.fori_loop(lo, hi, one, 0)
                lax.fori_loop(LATS - hi, LATS - lo, one, 0)

    def combine(depths, rows):
        first = 0
        for pair, depth in enumerate(depths):
            lo, hi = (16, 48) if pair >= 1 and len(depths) > 2 else (0, 64)
            data = got[lo:hi, :, pair * 128 : (pair + 1) * 128]
            data = data.reshape((hi - lo) * BLOCK, 128)
            both = [
                lax.dot_general(
                    basis[2 * pair + side, 0:depth, lo * BLOCK : hi * BLOCK],
                    data,
                    (((1,), (0,)), ((), ())),
                    preferred_element_type=F32,
                )
                for side in range(2)
            ]
            lane = lax.broadcasted_iota(jnp.int32, (depth, 128), 1)
            coef[first : first + depth, :] = jnp.where(lane < 64, both[0], both[1]).astype(BF16)
            first += depth
        coef[first:rows, :] = jnp.zeros((rows - first, 128), BF16)

    def month_copy(source, target, part):
        return pltpu.make_async_remote_copy(
            src_ref=coef.at[pl.ds(pl.multiple_of(target * part, part), part), :],
            dst_ref=share.at[source, pl.ds(0, part), :],
            send_sem=send_sem.at[1],
            recv_sem=month_sem.at[source],
            device_id={"tm": target},
            device_id_type=MESH,
        )

    def months(part):
        steps = (4, 3, 5, 2, 6, 1, 7)
        for step in steps:
            month_copy(tm, wrapped(tm + step, TMS), part).start()
        share[tm, 0:part, :] = coef[pl.ds(pl.multiple_of(tm * part, part), part), :]
        for step in steps[::-1]:
            month_copy(wrapped(tm + step, TMS), tm, part).wait_recv()
        pieces = [share[source, 0:part, :].astype(F32) for source in range(TMS)]
        columns = regroup(pieces).astype(BF16)
        terms = lax.dot_general(
            columns, columns, (((0,), (0,)), ((), ())), preferred_element_type=F32
        )
        row = lax.broadcasted_iota(jnp.int32, (MONTHS, MONTHS), 0)
        col = lax.broadcasted_iota(jnp.int32, (MONTHS, MONTHS), 1)
        squares = functools.reduce(jnp.add, [piece * piece for piece in pieces])
        trace = jnp.sum(jnp.sum(squares, axis=0, keepdims=True), axis=1, keepdims=True)
        spare = jnp.logical_and((row & 3) == 1, col == row - 1)
        terms = jnp.where(spare, trace, terms)
        for odd, value in enumerate(exchange_halves(terms[:, :128], terms[:, 128:])):
            gram[:, odd] = value.reshape(32, 8, 128)

    @pl.when(jnp.logical_not(inner))
    def _():
        tabulate(DEPTH_OUT)

        @pl.when(outer)
        def _():
            receive(False)

        combine(DEPTH_OUT, TMS * PART_OUT)
        months(PART_OUT)

    @pl.when(inner)
    def _():
        tabulate(DEPTH_IN)
        receive(True)
        combine(DEPTH_IN, TMS * PART_IN)
        months(PART_IN)

    me = tm * 8 + x * 2 + half
    y = tm // 2
    core = tm % 2
    plane = (z - half) * NX

    def slab_copy(source, target_y, target_core, target_x, target_half):
        target = target_y * 2 + target_core
        return pltpu.make_async_remote_copy(
            src_ref=gram.at[target * NX + target_x, target_half],
            dst_ref=slabs.at[source],
            send_sem=send_sem.at[2],
            recv_sem=slab_sem.at[source],
            device_id={"lat": plane + target_half * NX + target_x, "tm": target},
            device_id_type=MESH,
        )

    def others(away_first, action):
        order = (2, 1, 3, 0)
        for away_y in order if away_first else order[::-1]:
            peer_y = wrapped(y + away_y, 4)
            for away_x in order if away_first else order[::-1]:
                peer_x = wrapped(x + away_x, 4)
                for peer_half in (1 - half, half) if away_first else (half, 1 - half):
                    for peer_core in (1 - core, core):
                        here = away_y == 0 and away_x == 0
                        if not (here and peer_half is half and peer_core is core):
                            action(peer_y, peer_core, peer_x, peer_half)

    others(True, lambda *peer: slab_copy(me, *peer).start())
    slabs[me] = gram[me // 2, me % 2]

    def receive_slab(peer_y, peer_core, peer_x, peer_half):
        source = (peer_y * 2 + peer_core) * 8 + peer_x * 2 + peer_half
        slab_copy(source, y, core, x, half).wait_recv()

    others(False, receive_slab)
    own_pair = z // 2
    planes[own_pair] = jnp.sum(slabs[...], axis=0)

    def plane_copy(source, target):
        return pltpu.make_async_remote_copy(
            src_ref=planes.at[own_pair],
            dst_ref=planes.at[source],
            send_sem=send_sem.at[3],
            recv_sem=plane_sem.at[source],
            device_id={"lat": (target * 2 + half) * NX + x},
            device_id_type=MESH,
        )

    for away in (4, 3, 5, 2, 6, 1, 7):
        plane_copy(own_pair, wrapped(own_pair + away, 8)).start()

    each_row_copy(lambda copy: copy.wait_send())
    for applies, part in ((jnp.logical_not(inner), PART_OUT), (inner, PART_IN)):

        @pl.when(applies)
        def _(part=part):
            for step in range(1, TMS):
                month_copy(tm, wrapped(tm + step, TMS), part).wait_send()

    def slab_sent(step, carry):
        slab_copy(me, y, core, x, half).wait_send()
        return carry

    lax.fori_loop(1, 64, slab_sent, 0)

    for away in range(1, 8):
        plane_copy(wrapped(own_pair + away, 8), own_pair).wait_recv()
    slab = jnp.sum(planes[...], axis=0)
    later = me // 32
    row = lax.broadcasted_iota(jnp.int32, (8, 128), 0) - 4 * later
    col = lax.broadcasted_iota(jnp.int32, (8, 128), 1) - (4 * me - 128 * later)
    spare = jnp.logical_and(row == 1, col == 0)

    place = x * 2 + half
    finals[place] = jnp.where(spare, roll(roll(slab, 1, 0), -1, 1), slab)

    def last_copy(source, target):
        return pltpu.make_async_remote_copy(
            src_ref=finals.at[place],
            dst_ref=finals.at[source],
            send_sem=send_sem.at[4],
            recv_sem=last_sem.at[source],
            device_id={"lat": (z - half + target % 2) * NX + target // 2},
            device_id_type=MESH,
        )

    for away in (4, 5, 3, 2, 6, 1, 7):
        last_copy(place, wrapped(place + away, 8)).start()
    for away in range(1, 8):
        plane_copy(own_pair, wrapped(own_pair + away, 8)).wait_send()
    chosen = jnp.sum(jnp.where(spare, slab, 0.0), axis=0, keepdims=True)
    scale = MONTHS / (jnp.sum(chosen, axis=1, keepdims=True) + 1e-06)
    for away in range(1, 8):
        last_copy(wrapped(place + away, 8), place).wait_recv()
    for index in range(4):
        left, right = exchange_halves(finals[2 * index], finals[2 * index + 1])
        out_ref[8 * index : 8 * (index + 1), 0:128] = left * scale
        out_ref[8 * index : 8 * (index + 1), 128:256] = right * scale
    for away in range(1, 8):
        last_copy(place, wrapped(place + away, 8)).wait_send()


def local(fields):
    return pl.pallas_call(
        kernel,
        out_shape=jax.ShapeDtypeStruct((LOCAL, MONTHS), F32),
        in_specs=[pl.BlockSpec(memory_space=pltpu.HBM)],
        out_specs=pl.BlockSpec(memory_space=pltpu.VMEM),
        scratch_shapes=[
            pltpu.VMEM((BLOCK, LOCAL, NLON), BF16),
            pltpu.VMEM((2 * PAIRS, 8, NLON), F32),
            pltpu.VMEM((sum(pair_rows(PAIRS - 1)), NLON), BF16),
            pltpu.VMEM((PITCH_OUT // 2, 2, BLOCK, 256), BF16),
            pltpu.VMEM((PITCH_IN // 2, 2, BLOCK, LANES_IN), BF16),
            pltpu.VMEM((LATS, BLOCK, LANES_IN), BF16),
            pltpu.VMEM((4, 353 * 8, 128), F32),
            pltpu.VMEM((4, 33 * 8, 128), F32),
            pltpu.VMEM((10, 352, NLAT), BF16),
            pltpu.VMEM((TMS * PART_OUT, 128), BF16),
            pltpu.VMEM((TMS, PART_OUT, 128), BF16),
            pltpu.VMEM((32, 2, 8, 128), F32),
            pltpu.VMEM((64, 8, 128), F32),
            pltpu.VMEM((8, 8, 128), F32),
            pltpu.VMEM((8, 8, 128), F32),
            pltpu.SemaphoreType.DMA,
            pltpu.SemaphoreType.DMA((5,)),
            pltpu.SemaphoreType.DMA((LATS,)),
            pltpu.SemaphoreType.DMA((TMS,)),
            pltpu.SemaphoreType.DMA((64,)),
            pltpu.SemaphoreType.DMA((8,)),
            pltpu.SemaphoreType.DMA((8,)),
        ],
        compiler_params=pltpu.CompilerParams(
            collective_id=0, has_side_effects=True, vmem_limit_bytes=67_043_328
        ),
    )(fields)


def solution(mesh):
    return jax.shard_map(
        local,
        mesh=mesh,
        in_specs=(P("lat", "tm", None),),
        out_specs=P("tm", None),
        check_vma=False,
    )
```

```python
import functools
import math

import jax
import jax.numpy as jnp
from jax import lax
from jax.experimental import pallas as pl
from jax.experimental.pallas import tpu as pltpu
from jax.sharding import PartitionSpec as P

TRUNC = 341
NLON = 1024
NLAT = 512
MONTHS = 256
LATS = 64
TMS = 8
NX = 4
BLOCK = 8
LOCAL = 32
MIDDLE = 23
INNER = 16
IDLE = 2
OUTER = 46
FIRST_IN = 4 * OUTER
DEPTH_OUT = (352, 256)
DEPTH_IN = (160, 128, 96, 64, 32)
PART_OUT = 80
PART_IN = 64
PITCH_OUT = 48
PITCH_IN = 16
PAIRS_OUT = len(DEPTH_OUT)
PAIRS = PAIRS_OUT + len(DEPTH_IN)
LANES_IN = 128 * len(DEPTH_IN)
KINDS = (
    (0, 9, 128, 0),
    (9, 15, 256, 0),
    (15, 16, 256, 128),
    (16, 17, 256, 256),
    (17, 18, 256, 384),
    (18, 32, 256, 640),
)
MESH = pl.DeviceIdType.MESH
F32 = jnp.float32
BF16 = jnp.bfloat16
SINE = tuple(
    (-1.0) ** k * (2.0 * math.pi) ** (2 * k + 1) / math.factorial(2 * k + 1) for k in range(7)
)


def sine_of_turns(u):
    square = u * u
    total = jnp.full_like(u, SINE[6])
    for k in range(5, -1, -1):
        total = total * square + SINE[k]
    return total * u


def cosine_of_phase(phase):
    away = jnp.abs(((phase + 512) & 1023) - 512)
    return sine_of_turns((256 - away).astype(F32) * (1.0 / NLON))


def waves_times_lon(first, slot_step, owner_step, part_step):
    sub = lax.broadcasted_iota(jnp.int32, (8, NLON), 0)
    lon = lax.broadcasted_iota(jnp.int32, (8, NLON), 1)
    wave = first + slot_step * ((sub >> 1) & 1) + owner_step * (sub >> 2)
    return wave * lon + part_step * (sub & 1)


def cosine_sine(phase):
    return cosine_of_phase(phase), cosine_of_phase(phase - 256)


def turn(pair, by):
    cosine, sine = pair
    return cosine * by[0] - sine * by[1], sine * by[0] + cosine * by[1]


def roll(value, shift, axis):
    return pltpu.roll(value, shift % value.shape[axis], axis)


def swap_bit(value, bit):
    rows = value.shape[0]
    sub = (lax.broadcasted_iota(jnp.int32, (rows, 128), 0) >> bit) & 1
    group = (lax.broadcasted_iota(jnp.int32, (rows, 128), 1) >> (5 + bit)) & 1
    step = 1 << bit
    down = roll(value, 32 * step, 1)
    up = down if step == 2 else roll(value, -32 * step, 1)
    from_below = roll(down, -step, 0)
    from_above = roll(up, step, 0)
    return jnp.where(sub == group, value, jnp.where(sub == 0, from_below, from_above))


def rows_by_latitude(spectrum):
    low, high = spectrum[:, :128], spectrum[:, 128:]
    return [swap_bit(swap_bit(part, 0), 1) for part in exchange_halves(low, high)]


def start_value(order, sine_lat):
    ratio = jnp.ones_like(order)
    for step in range(1, 9):
        ratio = ratio * ((order + step) / (order + (step + 0.5)))
    far = order + 9.0
    inverse = 1.0 / far
    square = inverse * inverse
    series = inverse * (-1.0 / 8.0 + square * (1.0 / 192.0 - square * (1.0 / 640.0)))
    log_ratio = 0.5 * jnp.log(far) + series + jnp.log(ratio)
    constant = math.log(0.5) - (0.5 * math.log(math.pi) - math.log(2.0))
    log_start = 0.5 * (constant + log_ratio) + order * jnp.log(sine_lat)
    taper = jnp.clip((log_start + 70.0) / 10.0, 0.0, 1.0)
    return jnp.exp(jnp.maximum(log_start, -80.0)) * taper


def step_factors(order, degree):
    top = jnp.sqrt((4.0 * degree * degree - 1.0) / (degree * degree - order * order))
    below = degree - 1.0
    back = jnp.sqrt(
        jnp.maximum(below * below - order * order, 0.0) / jnp.abs(4.0 * below * below - 1.0)
    )
    return top, top * back


def legendre(waves, lane_offset):
    place = (lax.broadcasted_iota(jnp.int32, (8, 128), 1) + lane_offset).astype(F32) + 0.5
    turns = place * (0.5 / NLAT)
    folded = jnp.minimum(turns, 0.5 - turns)
    half = sine_of_turns(0.5 * folded)
    cosine = jnp.where(folded < 0.125, 1.0 - 2.0 * half * half, sine_of_turns(0.25 - folded))
    return jnp.where(turns < 0.25, cosine, -cosine), sine_of_turns(folded)


def lat_weight(width):
    turns = (lax.broadcasted_iota(jnp.int32, (1, width), 1).astype(F32) + 0.5) * (0.5 / NLAT)
    return sine_of_turns(jnp.minimum(turns, 0.5 - turns)) * (math.pi / NLAT)


def regroup(pieces):
    group = lax.broadcasted_iota(jnp.int32, pieces[0].shape, 1) >> 5
    blocks = []
    for g in range(4):
        halves = []
        for half in range(2):
            total = None
            for a in range(4):
                moved = pieces[4 * half + a]
                if a != g:
                    moved = roll(moved, 32 * (a - g), 1)
                total = moved if total is None else jnp.where(group == a, moved, total)
            halves.append(total)
        blocks.append(jnp.concatenate(halves, axis=1))
    return jnp.concatenate(blocks, axis=0)


def exchange_halves(left, right):
    upper = ((lax.broadcasted_iota(jnp.int32, left.shape, 0) >> 2) & 1) == 0
    return (
        jnp.where(upper, left, roll(right, 4, 0)),
        jnp.where(upper, roll(left, -4, 0), right),
    )


def wrapped(value, length):
    return jnp.where(value >= length, value - length, value)


def is_inner(lat):
    return jnp.logical_and(lat >= MIDDLE, lat < MIDDLE + INNER)


def is_outer(lat):
    return jnp.logical_or(lat < MIDDLE, lat >= MIDDLE + INNER + IDLE)


def outer_owner(lat):
    return jnp.where(lat < MIDDLE, lat, lat - INNER - IDLE)


def pair_rows(index):
    if index < PAIRS_OUT:
        return 4 * PITCH_OUT * index, 4 * PITCH_OUT
    return 4 * (PITCH_OUT * PAIRS_OUT + PITCH_IN * (index - PAIRS_OUT)), 4 * PITCH_IN


def kernel(
    fields_hbm,
    out_ref,
    fields,
    patterns,
    transform,
    send_out,
    send_in,
    got,
    values,
    more_values,
    basis,
    coef,
    share,
    gram,
    slabs,
    planes,
    finals,
    local_sem,
    send_sem,
    row_sem,
    month_sem,
    slab_sem,
    plane_sem,
    last_sem,
):
    lat = lax.axis_index("lat")
    tm = lax.axis_index("tm")
    z = lat // NX
    x = lat % NX
    half = z % 2
    inner = is_inner(lat)
    outer = is_outer(lat)
    load = pltpu.make_async_copy(fields_hbm, fields, local_sem)
    load.start()
    got[...] = jnp.zeros_like(got)

    barrier = pltpu.get_barrier_semaphore()
    for away in range(32, 0, -1):
        for step in {away, LATS - away}:
            pl.semaphore_signal(
                barrier,
                inc=1,
                device_id={"lat": wrapped(lat + step, LATS)},
                device_id_type=MESH,
            )
    for step in range(1, TMS):
        pl.semaphore_signal(
            barrier, inc=1, device_id={"tm": wrapped(tm + step, TMS)}, device_id_type=MESH
        )

    for index in range(PAIRS):
        if index < PAIRS_OUT:
            phase = waves_times_lon(2 * OUTER * index, OUTER, 0, 256)
        else:
            first = FIRST_IN + 2 * INNER * (index - PAIRS_OUT)
            phase = waves_times_lon(first, INNER, 0, 256)
        cosine, sine = cosine_sine(phase)
        patterns[2 * index] = cosine * (1.0 / math.sqrt(NLON))
        patterns[2 * index + 1] = sine * (1.0 / math.sqrt(NLON))
    by = cosine_sine(waves_times_lon(2, 0, 0, 0))

    def fill(kinds, trip, pair):
        following = turn(pair, by)
        for index in kinds:
            first, _ = pair_rows(index)
            rows = [
                cosine * patterns[2 * index] - sine * patterns[2 * index + 1]
                for cosine, sine in (pair, following)
            ]
            start = pl.multiple_of(first + trip * 16, 16)
            transform[pl.ds(start, 16), :] = jnp.concatenate(rows, axis=0).astype(BF16)
        return turn(following, by)

    pair = cosine_sine(waves_times_lon(0, 0, 1, 0))
    trips_in, trips_out = PITCH_IN // 4, PITCH_OUT // 4
    pair = lax.fori_loop(0, trips_in, functools.partial(fill, range(PAIRS)), pair)
    lax.fori_loop(trips_in, trips_out, functools.partial(fill, range(PAIRS_OUT)), pair)
    load.wait()
    flat = fields[...].reshape(BLOCK * LOCAL, NLON)
    for index in range(PAIRS):
        first, rows = pair_rows(index)
        if index < PAIRS_OUT:
            buffer, place = send_out, index
        else:
            buffer, place = send_in, index - PAIRS_OUT
        spectrum = lax.dot_general(
            transform[first : first + rows, :],
            flat,
            (((1,), (1,)), ((), ())),
            preferred_element_type=F32,
        )
        for odd, part in enumerate(rows_by_latitude(spectrum)):
            buffer[:, odd, :, place * 128 : (place + 1) * 128] = part.reshape(
                rows // 8, BLOCK, 128
            ).astype(BF16)

    own = jnp.where(inner, lat - MIDDLE, outer_owner(lat))

    @pl.when(inner)
    def _():
        got[lat] = send_in[own // 2, own % 2]

    @pl.when(outer)
    def _():
        got[lat, :, 0:256] = send_out[own // 2, own % 2]

    pl.semaphore_wait(barrier, LATS - 1 + TMS - 1)

    def row_copy(source, target, width, to_inner):
        if to_inner:
            peer = target - MIDDLE
            buffer = send_in
        else:
            peer = outer_owner(target)
            buffer = send_out
        return pltpu.make_async_remote_copy(
            src_ref=buffer.at[peer // 2, peer % 2, :, pl.ds(0, width)],
            dst_ref=got.at[source, :, pl.ds(0, width)],
            send_sem=send_sem.at[0],
            recv_sem=row_sem.at[source],
            device_id={"lat": target},
            device_id_type=MESH,
        )

    near = jnp.minimum(lat, LATS - 1 - lat)

    def each_row_copy(action):
        for lo, hi, width_out, width_in in KINDS:

            @pl.when(jnp.logical_and(near >= lo, near < hi))
            def _(width_out=width_out, width_in=width_in):
                def one(target, kind):
                    to_inner = is_inner(target)

                    if kind == 0:

                        @pl.when(is_outer(target))
                        def _():
                            action(row_copy(lat, target, width_out, False))

                    if width_in and kind == 1:

                        @pl.when(to_inner)
                        def _():
                            action(row_copy(lat, target, width_in, True))

                def both(kind, step, carry):
                    one(wrapped(lat + (32 - step), LATS), kind)
                    one(wrapped(lat + (32 + step), LATS), kind)
                    return carry

                for kind in (0, 1):
                    if kind == 0 or width_in:
                        one(wrapped(lat + 32, LATS), kind)
                        lax.fori_loop(1, 32, functools.partial(both, kind), 0)

    each_row_copy(lambda copy: copy.start())

    base = jnp.where(inner, FIRST_IN + own, jnp.where(outer, own, 400))
    stride = jnp.where(inner, INNER, OUTER)
    slot = jnp.minimum(
        lax.broadcasted_iota(jnp.int32, (8, 128), 0), jnp.where(inner, 7, 3)
    )
    order = (base + stride * slot).astype(F32)
    def recur(order, table, trips):
        cosines = []
        state = []
        for block in range(4):
            cosine_lat, sine_lat = legendre(order, 128 * block)
            cosines.append(cosine_lat)
            first = start_value(order, sine_lat)
            table[block, 0:8, :] = first
            state.append(first)
            state.append(jnp.zeros_like(first))

        def advance(trip, carry):
            carry = list(carry)
            for step in range(1, 9):
                offset = trip * 8 + step
                top, mixed = step_factors(order, order + offset.astype(F32))
                row = pl.multiple_of(offset * 8, 8)
                for block in range(4):
                    current, previous = carry[2 * block], carry[2 * block + 1]
                    following = top * cosines[block] * current - mixed * previous
                    table[block, pl.ds(row, 8), :] = following
                    carry[2 * block], carry[2 * block + 1] = following, current
            return tuple(carry)

        lax.fori_loop(0, trips, advance, tuple(state))

    recur(order, values, 44)

    @pl.when(inner)
    def _():
        slot = 8 + jnp.minimum(lax.broadcasted_iota(jnp.int32, (8, 128), 0), 1)
        recur((base + stride * slot).astype(F32), more_values, 4)

    weight = lat_weight(NLAT)

    def tabulate(depths):
        for slot in range(2 * len(depths)):
            depth = depths[slot // 2]
            wave = base + stride * slot
            factor = jnp.where(wave > 0, math.sqrt(2.0), 1.0).astype(F32)
            offset = lax.broadcasted_iota(jnp.int32, (depth, 128), 0)
            for block in range(4):
                lanes = slice(128 * block, 128 * (block + 1))
                source = values if slot < 8 else more_values
                table = source[block, pl.ds(slot % 8, depth, stride=8), :]
                table = jnp.where(
                    offset + wave <= TRUNC, table * (weight[:, lanes] * factor), 0.0
                )
                basis[slot, 0:depth, lanes] = table.astype(BF16)

    def receive(to_inner):
        for lo, hi, width_out, width_in in KINDS:
            width = width_in if to_inner else width_out
            if width:

                def one(source, carry, width=width):
                    @pl.when(source != lat)
                    def _():
                        row_copy(source, lat, width, to_inner).wait_recv()

                    return carry

                lax.fori_loop(lo, hi, one, 0)
                lax.fori_loop(LATS - hi, LATS - lo, one, 0)

    def combine(depths, rows):
        first = 0
        for pair, depth in enumerate(depths):
            lo, hi = (16, 48) if pair >= 1 and len(depths) > 2 else (0, 64)
            data = got[lo:hi, :, pair * 128 : (pair + 1) * 128]
            data = data.reshape((hi - lo) * BLOCK, 128)
            both = [
                lax.dot_general(
                    basis[2 * pair + side, 0:depth, lo * BLOCK : hi * BLOCK],
                    data,
                    (((1,), (0,)), ((), ())),
                    preferred_element_type=F32,
                )
                for side in range(2)
            ]
            lane = lax.broadcasted_iota(jnp.int32, (depth, 128), 1)
            coef[first : first + depth, :] = jnp.where(lane < 64, both[0], both[1]).astype(BF16)
            first += depth
        coef[first:rows, :] = jnp.zeros((rows - first, 128), BF16)

    def month_copy(source, target, part):
        return pltpu.make_async_remote_copy(
            src_ref=coef.at[pl.ds(pl.multiple_of(target * part, part), part), :],
            dst_ref=share.at[source, pl.ds(0, part), :],
            send_sem=send_sem.at[1],
            recv_sem=month_sem.at[source],
            device_id={"tm": target},
            device_id_type=MESH,
        )

    def months(part):
        steps = (4, 3, 5, 2, 6, 1, 7)
        for step in steps:
            month_copy(tm, wrapped(tm + step, TMS), part).start()
        share[tm, 0:part, :] = coef[pl.ds(pl.multiple_of(tm * part, part), part), :]
        for step in steps[::-1]:
            month_copy(wrapped(tm + step, TMS), tm, part).wait_recv()
        pieces = [share[source, 0:part, :].astype(F32) for source in range(TMS)]
        columns = regroup(pieces).astype(BF16)
        terms = lax.dot_general(
            columns, columns, (((0,), (0,)), ((), ())), preferred_element_type=F32
        )
        row = lax.broadcasted_iota(jnp.int32, (MONTHS, MONTHS), 0)
        col = lax.broadcasted_iota(jnp.int32, (MONTHS, MONTHS), 1)
        squares = functools.reduce(jnp.add, [piece * piece for piece in pieces])
        trace = jnp.sum(jnp.sum(squares, axis=0, keepdims=True), axis=1, keepdims=True)
        spare = jnp.logical_and((row & 3) == 1, col == row - 1)
        terms = jnp.where(spare, trace, terms)
        for odd, value in enumerate(exchange_halves(terms[:, :128], terms[:, 128:])):
            gram[:, odd] = value.reshape(32, 8, 128)

    @pl.when(jnp.logical_not(inner))
    def _():
        tabulate(DEPTH_OUT)

        @pl.when(outer)
        def _():
            receive(False)

        combine(DEPTH_OUT, TMS * PART_OUT)
        months(PART_OUT)

    @pl.when(inner)
    def _():
        tabulate(DEPTH_IN)
        receive(True)
        combine(DEPTH_IN, TMS * PART_IN)
        months(PART_IN)

    me = tm * 8 + x * 2 + half
    y = tm // 2
    core = tm % 2
    plane = (z - half) * NX

    def slab_copy(source, target_y, target_core, target_x, target_half):
        target = target_y * 2 + target_core
        return pltpu.make_async_remote_copy(
            src_ref=gram.at[target * NX + target_x, target_half],
            dst_ref=slabs.at[source],
            send_sem=send_sem.at[2],
            recv_sem=slab_sem.at[source],
            device_id={"lat": plane + target_half * NX + target_x, "tm": target},
            device_id_type=MESH,
        )

    def others(away_first, action):
        order = (2, 1, 3, 0)
        for away_y in order if away_first else order[::-1]:
            peer_y = wrapped(y + away_y, 4)
            for away_x in order if away_first else order[::-1]:
                peer_x = wrapped(x + away_x, 4)
                for peer_half in (1 - half, half) if away_first else (half, 1 - half):
                    for peer_core in (1 - core, core):
                        here = away_y == 0 and away_x == 0
                        if not (here and peer_half is half and peer_core is core):
                            action(peer_y, peer_core, peer_x, peer_half)

    others(True, lambda *peer: slab_copy(me, *peer).start())
    slabs[me] = gram[me // 2, me % 2]

    def receive_slab(peer_y, peer_core, peer_x, peer_half):
        source = (peer_y * 2 + peer_core) * 8 + peer_x * 2 + peer_half
        slab_copy(source, y, core, x, half).wait_recv()

    others(False, receive_slab)
    own_pair = z // 2
    planes[own_pair] = jnp.sum(slabs[...], axis=0)

    def plane_copy(source, target):
        return pltpu.make_async_remote_copy(
            src_ref=planes.at[own_pair],
            dst_ref=planes.at[source],
            send_sem=send_sem.at[3],
            recv_sem=plane_sem.at[source],
            device_id={"lat": (target * 2 + half) * NX + x},
            device_id_type=MESH,
        )

    for away in (4, 3, 5, 2, 6, 1, 7):
        plane_copy(own_pair, wrapped(own_pair + away, 8)).start()

    each_row_copy(lambda copy: copy.wait_send())
    for applies, part in ((jnp.logical_not(inner), PART_OUT), (inner, PART_IN)):

        @pl.when(applies)
        def _(part=part):
            for step in range(1, TMS):
                month_copy(tm, wrapped(tm + step, TMS), part).wait_send()

    def slab_sent(step, carry):
        slab_copy(me, y, core, x, half).wait_send()
        return carry

    lax.fori_loop(1, 64, slab_sent, 0)

    for away in range(1, 8):
        plane_copy(wrapped(own_pair + away, 8), own_pair).wait_recv()
    slab = jnp.sum(planes[...], axis=0)
    later = me // 32
    row = lax.broadcasted_iota(jnp.int32, (8, 128), 0) - 4 * later
    col = lax.broadcasted_iota(jnp.int32, (8, 128), 1) - (4 * me - 128 * later)
    spare = jnp.logical_and(row == 1, col == 0)

    place = x * 2 + half
    finals[place] = jnp.where(spare, roll(roll(slab, 1, 0), -1, 1), slab)

    def last_copy(source, target):
        return pltpu.make_async_remote_copy(
            src_ref=finals.at[place],
            dst_ref=finals.at[source],
            send_sem=send_sem.at[4],
            recv_sem=last_sem.at[source],
            device_id={"lat": (z - half + target % 2) * NX + target // 2},
            device_id_type=MESH,
        )

    for away in (4, 5, 3, 2, 6, 1, 7):
        last_copy(place, wrapped(place + away, 8)).start()
    for away in range(1, 8):
        plane_copy(own_pair, wrapped(own_pair + away, 8)).wait_send()
    chosen = jnp.sum(jnp.where(spare, slab, 0.0), axis=0, keepdims=True)
    scale = MONTHS / (jnp.sum(chosen, axis=1, keepdims=True) + 1e-06)
    for away in range(1, 8):
        last_copy(wrapped(place + away, 8), place).wait_recv()
    for index in range(4):
        left, right = exchange_halves(finals[2 * index], finals[2 * index + 1])
        out_ref[8 * index : 8 * (index + 1), 0:128] = left * scale
        out_ref[8 * index : 8 * (index + 1), 128:256] = right * scale
    for away in range(1, 8):
        last_copy(place, wrapped(place + away, 8)).wait_send()


def local(fields):
    return pl.pallas_call(
        kernel,
        out_shape=jax.ShapeDtypeStruct((LOCAL, MONTHS), F32),
        in_specs=[pl.BlockSpec(memory_space=pltpu.HBM)],
        out_specs=pl.BlockSpec(memory_space=pltpu.VMEM),
        scratch_shapes=[
            pltpu.VMEM((BLOCK, LOCAL, NLON), BF16),
            pltpu.VMEM((2 * PAIRS, 8, NLON), F32),
            pltpu.VMEM((sum(pair_rows(PAIRS - 1)), NLON), BF16),
            pltpu.VMEM((PITCH_OUT // 2, 2, BLOCK, 256), BF16),
            pltpu.VMEM((PITCH_IN // 2, 2, BLOCK, LANES_IN), BF16),
            pltpu.VMEM((LATS, BLOCK, LANES_IN), BF16),
            pltpu.VMEM((4, 353 * 8, 128), F32),
            pltpu.VMEM((4, 33 * 8, 128), F32),
            pltpu.VMEM((10, 352, NLAT), BF16),
            pltpu.VMEM((TMS * PART_OUT, 128), BF16),
            pltpu.VMEM((TMS, PART_OUT, 128), BF16),
            pltpu.VMEM((32, 2, 8, 128), F32),
            pltpu.VMEM((64, 8, 128), F32),
            pltpu.VMEM((8, 8, 128), F32),
            pltpu.VMEM((8, 8, 128), F32),
            pltpu.SemaphoreType.DMA,
            pltpu.SemaphoreType.DMA((5,)),
            pltpu.SemaphoreType.DMA((LATS,)),
            pltpu.SemaphoreType.DMA((TMS,)),
            pltpu.SemaphoreType.DMA((64,)),
            pltpu.SemaphoreType.DMA((8,)),
            pltpu.SemaphoreType.DMA((8,)),
        ],
        compiler_params=pltpu.CompilerParams(
            collective_id=0, has_side_effects=True, vmem_limit_bytes=67_043_328
        ),
    )(fields)


def solution(mesh):
    return jax.shard_map(
        local,
        mesh=mesh,
        in_specs=(P("lat", "tm", None),),
        out_specs=P("tm", None),
        check_vma=False,
    )
```

```python
import functools
import math

import jax
import jax.numpy as jnp
from jax import lax
from jax.experimental import pallas as pl
from jax.experimental.pallas import tpu as pltpu
from jax.sharding import PartitionSpec as P

TRUNC = 341
NLON = 1024
NLAT = 512
MONTHS = 256
LATS = 64
TMS = 8
NX = 4
BLOCK = 8
LOCAL = 32
MIDDLE = 23
INNER = 16
IDLE = 2
OUTER = 46
FIRST_IN = 4 * OUTER
DEPTH_OUT = (352, 256)
DEPTH_IN = (160, 128, 96, 64, 32)
PART_OUT = 80
PART_IN = 64
PITCH_OUT = 48
PITCH_IN = 16
PAIRS_OUT = len(DEPTH_OUT)
PAIRS = PAIRS_OUT + len(DEPTH_IN)
LANES_IN = 128 * len(DEPTH_IN)
KINDS = (
    (0, 9, 128, 0),
    (9, 15, 256, 0),
    (15, 16, 256, 128),
    (16, 17, 256, 256),
    (17, 18, 256, 384),
    (18, 32, 256, 640),
)
MESH = pl.DeviceIdType.MESH
F32 = jnp.float32
BF16 = jnp.bfloat16
SINE = tuple(
    (-1.0) ** k * (2.0 * math.pi) ** (2 * k + 1) / math.factorial(2 * k + 1) for k in range(7)
)


def sine_of_turns(u):
    square = u * u
    total = jnp.full_like(u, SINE[6])
    for k in range(5, -1, -1):
        total = total * square + SINE[k]
    return total * u


def cosine_of_phase(phase):
    away = jnp.abs(((phase + 512) & 1023) - 512)
    return sine_of_turns((256 - away).astype(F32) * (1.0 / NLON))


def waves_times_lon(first, slot_step, owner_step, part_step):
    sub = lax.broadcasted_iota(jnp.int32, (8, NLON), 0)
    lon = lax.broadcasted_iota(jnp.int32, (8, NLON), 1)
    wave = first + slot_step * ((sub >> 1) & 1) + owner_step * (sub >> 2)
    return wave * lon + part_step * (sub & 1)


def cosine_sine(phase):
    return cosine_of_phase(phase), cosine_of_phase(phase - 256)


def turn(pair, by):
    cosine, sine = pair
    return cosine * by[0] - sine * by[1], sine * by[0] + cosine * by[1]


def roll(value, shift, axis):
    return pltpu.roll(value, shift % value.shape[axis], axis)


def swap_bit(value, bit):
    rows = value.shape[0]
    sub = (lax.broadcasted_iota(jnp.int32, (rows, 128), 0) >> bit) & 1
    group = (lax.broadcasted_iota(jnp.int32, (rows, 128), 1) >> (5 + bit)) & 1
    step = 1 << bit
    down = roll(value, 32 * step, 1)
    up = down if step == 2 else roll(value, -32 * step, 1)
    from_below = roll(down, -step, 0)
    from_above = roll(up, step, 0)
    return jnp.where(sub == group, value, jnp.where(sub == 0, from_below, from_above))


def rows_by_latitude(spectrum):
    low, high = spectrum[:, :128], spectrum[:, 128:]
    return [swap_bit(swap_bit(part, 0), 1) for part in exchange_halves(low, high)]


def start_value(order, sine_lat):
    ratio = jnp.ones_like(order)
    for step in range(1, 9):
        ratio = ratio * ((order + step) / (order + (step + 0.5)))
    far = order + 9.0
    inverse = 1.0 / far
    square = inverse * inverse
    series = inverse * (-1.0 / 8.0 + square * (1.0 / 192.0 - square * (1.0 / 640.0)))
    log_ratio = 0.5 * jnp.log(far) + series + jnp.log(ratio)
    constant = math.log(0.5) - (0.5 * math.log(math.pi) - math.log(2.0))
    log_start = 0.5 * (constant + log_ratio) + order * jnp.log(sine_lat)
    taper = jnp.clip((log_start + 70.0) / 10.0, 0.0, 1.0)
    return jnp.exp(jnp.maximum(log_start, -80.0)) * taper


def step_factors(order, degree):
    top = jnp.sqrt((4.0 * degree * degree - 1.0) / (degree * degree - order * order))
    below = degree - 1.0
    back = jnp.sqrt(
        jnp.maximum(below * below - order * order, 0.0) / jnp.abs(4.0 * below * below - 1.0)
    )
    return top, top * back


def legendre(waves, lane_offset):
    place = (lax.broadcasted_iota(jnp.int32, (8, 128), 1) + lane_offset).astype(F32) + 0.5
    turns = place * (0.5 / NLAT)
    folded = jnp.minimum(turns, 0.5 - turns)
    half = sine_of_turns(0.5 * folded)
    cosine = jnp.where(folded < 0.125, 1.0 - 2.0 * half * half, sine_of_turns(0.25 - folded))
    return jnp.where(turns < 0.25, cosine, -cosine), sine_of_turns(folded)


def lat_weight(width):
    turns = (lax.broadcasted_iota(jnp.int32, (1, width), 1).astype(F32) + 0.5) * (0.5 / NLAT)
    return sine_of_turns(jnp.minimum(turns, 0.5 - turns)) * (math.pi / NLAT)


def regroup(pieces):
    group = lax.broadcasted_iota(jnp.int32, pieces[0].shape, 1) >> 5
    blocks = []
    for g in range(4):
        halves = []
        for half in range(2):
            total = None
            for a in range(4):
                moved = pieces[4 * half + a]
                if a != g:
                    moved = roll(moved, 32 * (a - g), 1)
                total = moved if total is None else jnp.where(group == a, moved, total)
            halves.append(total)
        blocks.append(jnp.concatenate(halves, axis=1))
    return jnp.concatenate(blocks, axis=0)


def exchange_halves(left, right):
    upper = ((lax.broadcasted_iota(jnp.int32, left.shape, 0) >> 2) & 1) == 0
    return (
        jnp.where(upper, left, roll(right, 4, 0)),
        jnp.where(upper, roll(left, -4, 0), right),
    )


def wrapped(value, length):
    return jnp.where(value >= length, value - length, value)


def is_inner(lat):
    return jnp.logical_and(lat >= MIDDLE, lat < MIDDLE + INNER)


def is_outer(lat):
    return jnp.logical_or(lat < MIDDLE, lat >= MIDDLE + INNER + IDLE)


def outer_owner(lat):
    return jnp.where(lat < MIDDLE, lat, lat - INNER - IDLE)


def pair_rows(index):
    if index < PAIRS_OUT:
        return 4 * PITCH_OUT * index, 4 * PITCH_OUT
    return 4 * (PITCH_OUT * PAIRS_OUT + PITCH_IN * (index - PAIRS_OUT)), 4 * PITCH_IN


def kernel(
    fields_hbm,
    out_ref,
    fields,
    patterns,
    transform,
    send_out,
    send_in,
    got,
    values,
    more_values,
    basis,
    coef,
    share,
    gram,
    slabs,
    planes,
    finals,
    local_sem,
    send_sem,
    row_sem,
    month_sem,
    slab_sem,
    plane_sem,
    last_sem,
):
    lat = lax.axis_index("lat")
    tm = lax.axis_index("tm")
    z = lat // NX
    x = lat % NX
    half = z % 2
    inner = is_inner(lat)
    outer = is_outer(lat)
    load = pltpu.make_async_copy(fields_hbm, fields, local_sem)
    load.start()
    got[...] = jnp.zeros_like(got)

    barrier = pltpu.get_barrier_semaphore()
    for away in range(32, 0, -1):
        for step in {away, LATS - away}:
            pl.semaphore_signal(
                barrier,
                inc=1,
                device_id={"lat": wrapped(lat + step, LATS)},
                device_id_type=MESH,
            )
    for step in range(1, TMS):
        pl.semaphore_signal(
            barrier, inc=1, device_id={"tm": wrapped(tm + step, TMS)}, device_id_type=MESH
        )

    for index in range(PAIRS):
        if index < PAIRS_OUT:
            phase = waves_times_lon(2 * OUTER * index, OUTER, 0, 256)
        else:
            first = FIRST_IN + 2 * INNER * (index - PAIRS_OUT)
            phase = waves_times_lon(first, INNER, 0, 256)
        cosine, sine = cosine_sine(phase)
        patterns[2 * index] = cosine * (1.0 / math.sqrt(NLON))
        patterns[2 * index + 1] = sine * (1.0 / math.sqrt(NLON))
    by = cosine_sine(waves_times_lon(2, 0, 0, 0))

    def fill(kinds, trip, pair):
        following = turn(pair, by)
        for index in kinds:
            first, _ = pair_rows(index)
            rows = [
                cosine * patterns[2 * index] - sine * patterns[2 * index + 1]
                for cosine, sine in (pair, following)
            ]
            start = pl.multiple_of(first + trip * 16, 16)
            transform[pl.ds(start, 16), :] = jnp.concatenate(rows, axis=0).astype(BF16)
        return turn(following, by)

    pair = cosine_sine(waves_times_lon(0, 0, 1, 0))
    trips_in, trips_out = PITCH_IN // 4, PITCH_OUT // 4
    pair = lax.fori_loop(0, trips_in, functools.partial(fill, range(PAIRS)), pair)
    lax.fori_loop(trips_in, trips_out, functools.partial(fill, range(PAIRS_OUT)), pair)
    load.wait()
    flat = fields[...].reshape(BLOCK * LOCAL, NLON)
    def transform_rows(indices):
        for index in indices:
            first, rows = pair_rows(index)
            if index < PAIRS_OUT:
                buffer, place = send_out, index
            else:
                buffer, place = send_in, index - PAIRS_OUT
            spectrum = lax.dot_general(
                transform[first : first + rows, :],
                flat,
                (((1,), (1,)), ((), ())),
                preferred_element_type=F32,
            )
            for odd, part in enumerate(rows_by_latitude(spectrum)):
                buffer[:, odd, :, place * 128 : (place + 1) * 128] = part.reshape(
                    rows // 8, BLOCK, 128
                ).astype(BF16)

    transform_rows(range(PAIRS_OUT))
    own = jnp.where(inner, lat - MIDDLE, outer_owner(lat))

    @pl.when(outer)
    def _():
        got[lat, :, 0:256] = send_out[own // 2, own % 2]

    pl.semaphore_wait(barrier, LATS - 1 + TMS - 1)

    def row_copy(source, target, width, to_inner):
        if to_inner:
            peer = target - MIDDLE
            buffer = send_in
        else:
            peer = outer_owner(target)
            buffer = send_out
        return pltpu.make_async_remote_copy(
            src_ref=buffer.at[peer // 2, peer % 2, :, pl.ds(0, width)],
            dst_ref=got.at[source, :, pl.ds(0, width)],
            send_sem=send_sem.at[0],
            recv_sem=row_sem.at[source],
            device_id={"lat": target},
            device_id_type=MESH,
        )

    near = jnp.minimum(lat, LATS - 1 - lat)

    def each_row_copy(action, kinds):
        for lo, hi, width_out, width_in in KINDS:

            @pl.when(jnp.logical_and(near >= lo, near < hi))
            def _(width_out=width_out, width_in=width_in):
                def one(target, kind):
                    to_inner = is_inner(target)

                    if kind == 0:

                        @pl.when(is_outer(target))
                        def _():
                            action(row_copy(lat, target, width_out, False))

                    if width_in and kind == 1:

                        @pl.when(to_inner)
                        def _():
                            action(row_copy(lat, target, width_in, True))

                def both(kind, step, carry):
                    one(wrapped(lat + (32 - step), LATS), kind)
                    one(wrapped(lat + (32 + step), LATS), kind)
                    return carry

                for kind in kinds:
                    if kind == 0 or width_in:
                        one(wrapped(lat + 32, LATS), kind)
                        lax.fori_loop(1, 32, functools.partial(both, kind), 0)

    each_row_copy(lambda copy: copy.start(), (0,))
    transform_rows(range(PAIRS_OUT, PAIRS))
    each_row_copy(lambda copy: copy.start(), (1,))

    @pl.when(inner)
    def _():
        got[lat] = send_in[own // 2, own % 2]

    base = jnp.where(inner, FIRST_IN + own, jnp.where(outer, own, 400))
    stride = jnp.where(inner, INNER, OUTER)
    slot = jnp.minimum(
        lax.broadcasted_iota(jnp.int32, (8, 128), 0), jnp.where(inner, 7, 3)
    )
    order = (base + stride * slot).astype(F32)
    def recur(order, table, trips):
        cosines = []
        state = []
        for block in range(4):
            cosine_lat, sine_lat = legendre(order, 128 * block)
            cosines.append(cosine_lat)
            first = start_value(order, sine_lat)
            table[block, 0:8, :] = first
            state.append(first)
            state.append(jnp.zeros_like(first))

        def advance(trip, carry):
            carry = list(carry)
            for step in range(1, 9):
                offset = trip * 8 + step
                top, mixed = step_factors(order, order + offset.astype(F32))
                row = pl.multiple_of(offset * 8, 8)
                for block in range(4):
                    current, previous = carry[2 * block], carry[2 * block + 1]
                    following = top * cosines[block] * current - mixed * previous
                    table[block, pl.ds(row, 8), :] = following
                    carry[2 * block], carry[2 * block + 1] = following, current
            return tuple(carry)

        lax.fori_loop(0, trips, advance, tuple(state))

    recur(order, values, 44)

    @pl.when(inner)
    def _():
        slot = 8 + jnp.minimum(lax.broadcasted_iota(jnp.int32, (8, 128), 0), 1)
        recur((base + stride * slot).astype(F32), more_values, 4)

    weight = lat_weight(NLAT)

    def tabulate(depths):
        for slot in range(2 * len(depths)):
            depth = depths[slot // 2]
            wave = base + stride * slot
            factor = jnp.where(wave > 0, math.sqrt(2.0), 1.0).astype(F32)
            offset = lax.broadcasted_iota(jnp.int32, (depth, 128), 0)
            for block in range(4):
                lanes = slice(128 * block, 128 * (block + 1))
                source = values if slot < 8 else more_values
                table = source[block, pl.ds(slot % 8, depth, stride=8), :]
                table = jnp.where(
                    offset + wave <= TRUNC, table * (weight[:, lanes] * factor), 0.0
                )
                basis[slot, 0:depth, lanes] = table.astype(BF16)

    def receive(to_inner):
        for lo, hi, width_out, width_in in KINDS:
            width = width_in if to_inner else width_out
            if width:

                def one(source, carry, width=width):
                    @pl.when(source != lat)
                    def _():
                        row_copy(source, lat, width, to_inner).wait_recv()

                    return carry

                lax.fori_loop(lo, hi, one, 0)
                lax.fori_loop(LATS - hi, LATS - lo, one, 0)

    def combine(depths, rows):
        first = 0
        for pair, depth in enumerate(depths):
            lo, hi = (16, 48) if pair >= 1 and len(depths) > 2 else (0, 64)
            data = got[lo:hi, :, pair * 128 : (pair + 1) * 128]
            data = data.reshape((hi - lo) * BLOCK, 128)
            both = [
                lax.dot_general(
                    basis[2 * pair + side, 0:depth, lo * BLOCK : hi * BLOCK],
                    data,
                    (((1,), (0,)), ((), ())),
                    preferred_element_type=F32,
                )
                for side in range(2)
            ]
            lane = lax.broadcasted_iota(jnp.int32, (depth, 128), 1)
            coef[first : first + depth, :] = jnp.where(lane < 64, both[0], both[1]).astype(BF16)
            first += depth
        coef[first:rows, :] = jnp.zeros((rows - first, 128), BF16)

    def month_copy(source, target, part):
        return pltpu.make_async_remote_copy(
            src_ref=coef.at[pl.ds(pl.multiple_of(target * part, part), part), :],
            dst_ref=share.at[source, pl.ds(0, part), :],
            send_sem=send_sem.at[1],
            recv_sem=month_sem.at[source],
            device_id={"tm": target},
            device_id_type=MESH,
        )

    def months(part):
        steps = (4, 3, 5, 2, 6, 1, 7)
        for step in steps:
            month_copy(tm, wrapped(tm + step, TMS), part).start()
        share[tm, 0:part, :] = coef[pl.ds(pl.multiple_of(tm * part, part), part), :]
        pieces = []
        for source in range(TMS):

            @pl.when(source != tm)
            def _(source=source):
                month_copy(source, tm, part).wait_recv()

            pieces.append(share[source, 0:part, :].astype(F32))
        columns = regroup(pieces).astype(BF16)
        terms = lax.dot_general(
            columns, columns, (((0,), (0,)), ((), ())), preferred_element_type=F32
        )
        row = lax.broadcasted_iota(jnp.int32, (MONTHS, MONTHS), 0)
        col = lax.broadcasted_iota(jnp.int32, (MONTHS, MONTHS), 1)
        squares = functools.reduce(jnp.add, [piece * piece for piece in pieces])
        trace = jnp.sum(jnp.sum(squares, axis=0, keepdims=True), axis=1, keepdims=True)
        spare = jnp.logical_and((row & 3) == 1, col == row - 1)
        terms = jnp.where(spare, trace, terms)
        for odd, value in enumerate(exchange_halves(terms[:, :128], terms[:, 128:])):
            gram[:, odd] = value.reshape(32, 8, 128)

    @pl.when(jnp.logical_not(inner))
    def _():
        tabulate(DEPTH_OUT)

        @pl.when(outer)
        def _():
            receive(False)

        combine(DEPTH_OUT, TMS * PART_OUT)
        months(PART_OUT)

    @pl.when(inner)
    def _():
        tabulate(DEPTH_IN)
        receive(True)
        combine(DEPTH_IN, TMS * PART_IN)
        months(PART_IN)

    me = tm * 8 + x * 2 + half
    y = tm // 2
    core = tm % 2
    plane = (z - half) * NX

    def slab_copy(source, target_y, target_core, target_x, target_half):
        target = target_y * 2 + target_core
        return pltpu.make_async_remote_copy(
            src_ref=gram.at[target * NX + target_x, target_half],
            dst_ref=slabs.at[source],
            send_sem=send_sem.at[2],
            recv_sem=slab_sem.at[source],
            device_id={"lat": plane + target_half * NX + target_x, "tm": target},
            device_id_type=MESH,
        )

    def others(away_first, action):
        places = sorted(
            ((i, j) for i in range(4) for j in range(4)),
            key=lambda place: sum(min(k, 4 - k) for k in place),
            reverse=away_first,
        )
        for away_y, away_x in places:
            peer_y = wrapped(y + away_y, 4)
            peer_x = wrapped(x + away_x, 4)
            for peer_half in (1 - half, half) if away_first else (half, 1 - half):
                for peer_core in (1 - core, core):
                    here = away_y == 0 and away_x == 0
                    if not (here and peer_half is half and peer_core is core):
                        action(peer_y, peer_core, peer_x, peer_half)

    others(True, lambda *peer: slab_copy(me, *peer).start())
    slabs[me] = gram[me // 2, me % 2]

    def receive_slab(peer_y, peer_core, peer_x, peer_half):
        source = (peer_y * 2 + peer_core) * 8 + peer_x * 2 + peer_half
        slab_copy(source, y, core, x, half).wait_recv()

    others(False, receive_slab)
    own_pair = z // 2
    planes[own_pair] = jnp.sum(slabs[...], axis=0)

    def plane_copy(source, target):
        return pltpu.make_async_remote_copy(
            src_ref=planes.at[own_pair],
            dst_ref=planes.at[source],
            send_sem=send_sem.at[3],
            recv_sem=plane_sem.at[source],
            device_id={"lat": (target * 2 + half) * NX + x},
            device_id_type=MESH,
        )

    for away in (4, 3, 5, 2, 6, 1, 7):
        plane_copy(own_pair, wrapped(own_pair + away, 8)).start()

    each_row_copy(lambda copy: copy.wait_send(), (0, 1))
    for applies, part in ((jnp.logical_not(inner), PART_OUT), (inner, PART_IN)):

        @pl.when(applies)
        def _(part=part):
            for step in range(1, TMS):
                month_copy(tm, wrapped(tm + step, TMS), part).wait_send()

    def slab_sent(step, carry):
        slab_copy(me, y, core, x, half).wait_send()
        return carry

    lax.fori_loop(1, 64, slab_sent, 0)

    for away in range(1, 8):
        plane_copy(wrapped(own_pair + away, 8), own_pair).wait_recv()
    slab = jnp.sum(planes[...], axis=0)
    later = me // 32
    row = lax.broadcasted_iota(jnp.int32, (8, 128), 0) - 4 * later
    col = lax.broadcasted_iota(jnp.int32, (8, 128), 1) - (4 * me - 128 * later)
    spare = jnp.logical_and(row == 1, col == 0)

    place = x * 2 + half
    finals[place] = jnp.where(spare, roll(roll(slab, 1, 0), -1, 1), slab)

    def last_copy(source, target):
        return pltpu.make_async_remote_copy(
            src_ref=finals.at[place],
            dst_ref=finals.at[source],
            send_sem=send_sem.at[4],
            recv_sem=last_sem.at[source],
            device_id={"lat": (z - half + target % 2) * NX + target // 2},
            device_id_type=MESH,
        )

    for away in (4, 5, 3, 2, 6, 1, 7):
        last_copy(place, wrapped(place + away, 8)).start()
    for away in range(1, 8):
        plane_copy(own_pair, wrapped(own_pair + away, 8)).wait_send()
    chosen = jnp.sum(jnp.where(spare, slab, 0.0), axis=0, keepdims=True)
    scale = MONTHS / (jnp.sum(chosen, axis=1, keepdims=True) + 1e-06)
    for away in range(1, 8):
        last_copy(wrapped(place + away, 8), place).wait_recv()
    for index in range(4):
        left, right = exchange_halves(finals[2 * index], finals[2 * index + 1])
        out_ref[8 * index : 8 * (index + 1), 0:128] = left * scale
        out_ref[8 * index : 8 * (index + 1), 128:256] = right * scale
    for away in range(1, 8):
        last_copy(place, wrapped(place + away, 8)).wait_send()


def local(fields):
    return pl.pallas_call(
        kernel,
        out_shape=jax.ShapeDtypeStruct((LOCAL, MONTHS), F32),
        in_specs=[pl.BlockSpec(memory_space=pltpu.HBM)],
        out_specs=pl.BlockSpec(memory_space=pltpu.VMEM),
        scratch_shapes=[
            pltpu.VMEM((BLOCK, LOCAL, NLON), BF16),
            pltpu.VMEM((2 * PAIRS, 8, NLON), F32),
            pltpu.VMEM((sum(pair_rows(PAIRS - 1)), NLON), BF16),
            pltpu.VMEM((PITCH_OUT // 2, 2, BLOCK, 256), BF16),
            pltpu.VMEM((PITCH_IN // 2, 2, BLOCK, LANES_IN), BF16),
            pltpu.VMEM((LATS, BLOCK, LANES_IN), BF16),
            pltpu.VMEM((4, 353 * 8, 128), F32),
            pltpu.VMEM((4, 33 * 8, 128), F32),
            pltpu.VMEM((10, 352, NLAT), BF16),
            pltpu.VMEM((TMS * PART_OUT, 128), BF16),
            pltpu.VMEM((TMS, PART_OUT, 128), BF16),
            pltpu.VMEM((32, 2, 8, 128), F32),
            pltpu.VMEM((64, 8, 128), F32),
            pltpu.VMEM((8, 8, 128), F32),
            pltpu.VMEM((8, 8, 128), F32),
            pltpu.SemaphoreType.DMA,
            pltpu.SemaphoreType.DMA((5,)),
            pltpu.SemaphoreType.DMA((LATS,)),
            pltpu.SemaphoreType.DMA((TMS,)),
            pltpu.SemaphoreType.DMA((64,)),
            pltpu.SemaphoreType.DMA((8,)),
            pltpu.SemaphoreType.DMA((8,)),
        ],
        compiler_params=pltpu.CompilerParams(
            collective_id=0, has_side_effects=True, vmem_limit_bytes=67_043_328
        ),
    )(fields)


def solution(mesh):
    return jax.shard_map(
        local,
        mesh=mesh,
        in_specs=(P("lat", "tm", None),),
        out_specs=P("tm", None),
        check_vma=False,
    )
```
